512 devices in a mesh: lat: 128 (over y, x_lo, z), lev: 4 (over x_hi, core).
Axes of the slice: x: 4 (x_hi: 2, x_lo: 2; x = x_hi * 2 + x_lo), y: 8, z: 8, core: 2. Of those that a mesh axis runs over, the one named last changes fastest.
Arguments:
- assign: int32 [640], replicated, may hold values from 0 to 639, each once
- u_spec: bfloat16 [640, 32, 2, 640], P('lat', 'lev'), may hold values from -0.25 to 0.25
- v_spec: bfloat16 [640, 32, 2, 640], P('lat', 'lev'), may hold values from -0.25 to 0.25
- basis: bfloat16 [640, 640, 640], P('lat', 'lev'), may hold values from -0.25 to 0.25
Outputs:
- vort_spec: float32 [640, 32, 2, 640], P('lat', 'lev')
The draws below stay inside these ranges and needn't reach their ends.
Inputs may be any that keep to these rules, and one draw needn't show every extreme that they name: Row k of u_spec, v_spec, basis and vort_spec belongs to zonal wavenumber assign[k]; each of the 640 wavenumbers appears once.
All inputs are finite; a program needn't handle non-finite values.
Results may differ from the reference program's by a relative error of at most 0.0061.
Values may be sent and summed in bfloat16 or wider, within the bound.
A program may use at most 64 MiB of HBM per device.

```python
import math
import jax
import jax.numpy as jnp
from jax import lax

M = 640
LAT = 1280
LON = 2560
LEVELS = 32
HALF = 640


def block_levels(stream_key, extent, shards, smallest, high):
    def one(position, blocks):
        steps = jax.random.uniform(jax.random.fold_in(jax.random.fold_in(stream_key, 6), position), (blocks,), jnp.float32, smallest / len(shards), high / len(shards))
        return jnp.repeat(jnp.exp(steps), extent[position] // blocks).reshape((-1,) + (1,) * (len(extent) - position - 1))

    factor_of = one(*shards[0])
    for cut in shards[1:]:
        factor_of = factor_of * one(*cut)
    return factor_of


def gaussian(key, extent, scale, bound, split=(), kind=jnp.bfloat16):
    drawn = scale * jax.random.normal(key, extent, jnp.float32)
    if split:
        drawn = drawn * block_levels(key, extent, split, -0.22, 0.18)
    return jnp.clip(drawn, -bound, bound).astype(kind)


def setup_inputs(seed: int = 0) -> dict:
    splits = jax.random.split(jax.random.key(seed), 5)
    assign = jax.random.permutation(splits[0], M).astype(jnp.int32)
    u_spec = gaussian(splits[1], (M, LEVELS, 2, M), M ** -0.5, 0.25, ((0, 128), (1, 4)))
    v_spec = gaussian(splits[2], (M, LEVELS, 2, M), M ** -0.5, 0.25, ((0, 128), (1, 4)))
    basis = gaussian(splits[3], (M, HALF, M), M ** -0.5, 0.25, ((0, 128), (1, 4)))
    return {"assign": assign, "u_spec": u_spec, "v_spec": v_spec, "basis": basis}


def degree_factors(wavenums):
    degree = jnp.arange(M, dtype=jnp.int32)
    live_mask = (degree[None, :] >= wavenums[:, None]).astype(jnp.int32)
    parity = 1 - 2 * ((degree[None, :] + wavenums[:, None]) % 2)
    return (live_mask, live_mask * parity)

def zonal_tables(wavenums):
    columns = jnp.arange(LON, dtype=jnp.int32)
    phases = wavenums[:, None] * columns[None, :] % LON
    angles = phases.astype(jnp.float32) * (2.0 * math.pi / LON)
    return jnp.stack([jnp.cos(angles), jnp.sin(angles)], axis=0).astype(jnp.bfloat16)

def reference(assign, u_spec, v_spec, basis):
    assign = assign.astype(jnp.int32)
    half_rows = LAT // 2
    live_mask, signed = degree_factors(assign)
    spectra = jnp.stack([u_spec, v_spec], axis=2).reshape(M, LEVELS * 4, M)

    def meridional(inputs):
        coeffs, live_row, signed_row, legendre = inputs
        masked = coeffs * live_row.astype(jnp.bfloat16)[None, :]
        flipped = coeffs * signed_row.astype(jnp.bfloat16)[None, :]
        northern = jnp.dot(legendre, masked.T, preferred_element_type=jnp.float32)
        southern = jnp.dot(legendre, flipped.T, preferred_element_type=jnp.float32)[::-1]
        return jnp.concatenate([northern, southern], axis=0).astype(jnp.bfloat16)
    fourier = lax.map(meridional, (spectra, live_mask, signed, basis))
    per_level = fourier.reshape(M, LAT, LEVELS, 2, 2).transpose(2, 0, 1, 3, 4)
    wave_f = zonal_tables(assign).astype(jnp.float32)
    inv_root = 1.0 / math.sqrt(LON)

    def zonal_section(level_block):
        grid_fields = jnp.einsum('kjfc,ckq->fjq', level_block.astype(jnp.float32), wave_f)
        scaled = grid_fields[0]
        upper_row = -jnp.roll(scaled[0], LON // 2, axis=-1)
        lower_row = -jnp.roll(scaled[-1], LON // 2, axis=-1)
        extended = jnp.concatenate([upper_row[None], scaled, lower_row[None]], axis=0)
        merid_v = grid_fields[1]
        vorticity = 0.5 * (jnp.roll(merid_v, -1, axis=-1) - jnp.roll(merid_v, 1, axis=-1)) - 0.5 * (extended[:-2] - extended[2:])
        flux = (vorticity * scaled).astype(jnp.bfloat16)
        zonal_back = jnp.einsum('jq,ckq->kjc', flux.astype(jnp.float32), wave_f) * inv_root
        return zonal_back.astype(jnp.bfloat16)
    zonal = lax.map(zonal_section, per_level)
    zonal = zonal.transpose(1, 2, 0, 3).reshape(M, LAT, LEVELS * 2)

    def project(inputs):
        returned, live_row, signed_row, legendre = inputs
        northern = jnp.dot(legendre.T, returned[:half_rows], preferred_element_type=jnp.float32)
        southern = jnp.dot(legendre.T, returned[half_rows:][::-1], preferred_element_type=jnp.float32)
        combined = live_row.astype(jnp.float32)[:, None] * northern + signed_row.astype(jnp.float32)[:, None] * southern
        return combined.reshape(M, LEVELS, 2).transpose(1, 2, 0)
    return lax.map(project, (zonal, live_mask, signed, basis))
```

```python
import functools
import math

import jax
import jax.numpy as jnp
from jax import lax
from jax.experimental import pallas as pl
from jax.experimental.pallas import tpu as pltpu
from jax.sharding import PartitionSpec as P

LON = 2560
SLOTS = 5
BLOCKS = 5
LANES = 128
PARTNER_CORE = [(0, 1), (1, 0), (2, 3), (3, 2)]
PARTNER_X = [(0, 2), (2, 0), (1, 3), (3, 1)]


def cos_sin(turns):
    x = turns - jnp.floor(turns + 0.5)
    u = x * x
    cos = jnp.full_like(u, (2 * math.pi) ** 18 / math.factorial(18) * -1.0)
    sin = jnp.full_like(u, (2 * math.pi) ** 19 / math.factorial(19) * -1.0)
    for i in range(8, -1, -1):
        sign = 1.0 if i % 2 == 0 else -1.0
        cos = cos * u + sign * (2 * math.pi) ** (2 * i) / math.factorial(2 * i)
        sin = sin * u + sign * (2 * math.pi) ** (2 * i + 1) / math.factorial(2 * i + 1)
    return cos, sin * x


def kernel(
    n_lat, rows_x, levels, degrees,
    waves_ref, factors_ref, lhs_ref, basis_ref, lane_waves_ref, row_waves_ref,
    out_ref,
    send, recv, coeffs, flux, back, ret, sum_send, sum_recv, table_q, table_k,
    send_sem, recv_sem, local_sem, back_send_sem, back_recv_sem, back_local_sem, sum_send_sem, sum_recv_sem,
):
    me = lax.axis_index("lat")
    lev = lax.axis_index("lev")
    x_hi = lev // 2
    groups = n_lat // 8
    units = BLOCKS * levels
    pair = 2 * levels
    spread = 2 * lev
    wide = basis_ref.shape[1]
    total = SLOTS * n_lat * 2

    my_group = me // 8
    my_z = lax.rem(lax.rem(me, 8) + 32 - lax.rem(my_group * 3 + spread, 8), 8)
    my_entry = (5 * my_z + 7) // 8
    active = (8 * my_entry) // 5 == my_z
    my_unit = my_group * 5 + my_entry
    my_block = my_unit // levels
    my_level = lax.rem(my_unit, levels)

    def owner_of(unit):
        group = unit // 5
        entry = lax.rem(unit, 5)
        return group * 8 + lax.rem((8 * entry) // 5 + lax.rem(group * 3 + spread, 8), 8)

    barrier = pltpu.get_barrier_semaphore()

    @pl.loop(1, n_lat)
    def _(i):
        pl.semaphore_signal(barrier, inc=1, device_id={"lat": lax.rem(me + i, n_lat)}, device_id_type=pl.DeviceIdType.MESH)

    partner = lax.rem(lev + 2, 4)
    pl.semaphore_signal(barrier, inc=1, device_id={"lev": partner}, device_id_type=pl.DeviceIdType.MESH)

    send_rows = send.reshape(2, BLOCKS, SLOTS, pair, LANES)
    lane = lax.broadcasted_iota(jnp.int32, (2 * pair, wide), 1)
    row = lax.broadcasted_iota(jnp.int32, (2 * pair, wide), 0)
    half_sign = jnp.where(row < pair, -0.5, 0.5)
    lane_tile = lax.broadcasted_iota(jnp.int32, (pair, LANES), 1)

    @pl.loop(0, SLOTS)
    def _(k):
        fields = lax.dot_general(
            lhs_ref[k], basis_ref[k], (((1,), (1,)), ((), ())), preferred_element_type=jnp.float32
        )
        wind = fields[: 2 * pair]
        other = fields[2 * pair :]
        before = pltpu.roll(wind, 1, 1)
        after = pltpu.roll(wind, wide - 1, 1)
        swapped = jnp.concatenate([wind[pair:], wind[:pair]], axis=0)
        before = jnp.where((lane == 0) & (x_hi == 0), -factors_ref[1, k] * wind, before)
        after = jnp.where((lane == rows_x - 1) & (x_hi == 1), swapped, after)
        curl = factors_ref[0, k] * other + half_sign * (before - after)
        for f, value in enumerate((wind, curl)):
            north, south = value[:pair], value[pair:]
            tail = 2 * LANES
            mixed = jnp.where(
                lane_tile < LANES // 2,
                north[:, tail : tail + LANES],
                pltpu.roll(south[:, tail : tail + LANES], LANES // 2, 1),
            )
            tiles = (north[:, :LANES], north[:, LANES:tail], south[:, :LANES], south[:, LANES:tail], mixed)
            for b, tile in enumerate(tiles):
                send_rows[f, b, k] = tile.astype(jnp.bfloat16)

    chunk = min(64, total)

    @pl.loop(0, total // chunk)
    def _(i):
        rows = pl.ds(pl.multiple_of(i * chunk, chunk), chunk)
        wave = row_waves_ref[rows, :]
        column = lax.broadcasted_iota(jnp.int32, (chunk, LANES), 1).astype(jnp.float32)
        part = lax.broadcasted_iota(jnp.int32, (chunk, LANES), 0)
        shift = (part - 2 * (part // 2)).astype(jnp.float32) * 0.25
        cos, sin = cos_sin(wave * column * (1.0 / LON) - shift)
        turn_cos, turn_sin = cos_sin(wave * (LANES / LON))
        for step in range(LON // LANES):
            table_k[rows, step * LANES : (step + 1) * LANES] = cos.astype(jnp.bfloat16)
            cos, sin = cos * turn_cos - sin * turn_sin, sin * turn_cos + cos * turn_sin

    pl.semaphore_wait(barrier, n_lat)

    first = (me * 5) // 8

    def unit_copy(unit):
        block = unit // levels
        level = lax.rem(unit, levels)
        return send.at[:, block, :, level], owner_of(unit)

    @pl.loop(0, units)
    def _(i):
        unit = lax.rem(first + i, units)
        source, owner = unit_copy(unit)

        @pl.when(owner != me)
        def _():
            pltpu.make_async_remote_copy(
                src_ref=source, dst_ref=recv.at[:, me], send_sem=send_sem, recv_sem=recv_sem,
                device_id={"lat": owner}, device_id_type=pl.DeviceIdType.MESH,
            ).start()

        @pl.when(owner == me)
        def _():
            pltpu.make_async_copy(source, recv.at[:, me], local_sem).start()

    width = total // 2
    for part in range(2):
        lanes = pl.ds(part * width, width)
        height = 16
        wave = jnp.broadcast_to(lane_waves_ref[0:1, lanes], (height, width))
        position = lax.broadcasted_iota(jnp.int32, (height, width), 0).astype(jnp.float32)
        side = lax.broadcasted_iota(jnp.int32, (height, width), 1)
        shift = (side - 2 * (side // 2)).astype(jnp.float32) * 0.25
        start = cos_sin(wave * position * (1.0 / LON) - shift)
        turn_cos, turn_sin = cos_sin(lane_waves_ref[0:8, lanes] * (height / LON))
        turn_cos = jnp.concatenate([turn_cos] * (height // 8), axis=0)
        turn_sin = jnp.concatenate([turn_sin] * (height // 8), axis=0)

        def advance(i, carry):
            cos, sin = carry
            table_q[pl.ds(pl.multiple_of(i * height, height), height), lanes] = cos.astype(jnp.bfloat16)
            return cos * turn_cos - sin * turn_sin, sin * turn_cos + cos * turn_sin

        lax.fori_loop(0, LON // height, advance, start)

    @pl.when(active)
    def _():
        remote = recv.at[:, pl.ds(0, n_lat - 1)]
        pltpu.make_async_copy(remote, remote, recv_sem).wait()
        pltpu.make_async_copy(recv.at[:, 0], recv.at[:, 0], local_sem).wait()
        recv_rows = recv.reshape(2, total, LANES)
        coeffs[:, :LANES] = recv_rows[0]
        coeffs[:, LANES:] = recv_rows[1]
        step = 256

        @pl.loop(0, LON // step)
        def _(i):
            rows = pl.ds(pl.multiple_of(i * step, step), step)
            grid = jnp.dot(table_q[rows, :], coeffs[...], preferred_element_type=jnp.float32)
            flux[rows, :] = (grid[:, :LANES] * grid[:, LANES:]).astype(jnp.bfloat16)

        back_rows = back.reshape(total, LANES)
        high = min(256, total)

        @pl.loop(0, total // high)
        def _(i):
            rows = pl.ds(pl.multiple_of(i * high, high), high)
            zonal = jnp.dot(table_k[rows, :], flux[...], preferred_element_type=jnp.float32)
            back_rows[rows, :] = (zonal * (1.0 / math.sqrt(LON))).astype(jnp.bfloat16)

        @pl.loop(1, n_lat)
        def _(i):
            owner = lax.rem(me + i, n_lat)
            pltpu.make_async_remote_copy(
                src_ref=back.at[owner], dst_ref=ret.at[my_block, :, my_level],
                send_sem=back_send_sem, recv_sem=back_recv_sem,
                device_id={"lat": owner}, device_id_type=pl.DeviceIdType.MESH,
            ).start()

        own = pltpu.make_async_copy(back.at[me], ret.at[my_block, :, my_level], back_local_sem)
        own.start()
        own.wait()
        sent = recv.at[:, pl.ds(0, units - 1)]
        pltpu.make_async_copy(sent, sent, send_sem).wait()
        got = recv.at[0, pl.ds(0, units - 1)]
        pltpu.make_async_copy(got, got, back_recv_sem).wait()

    @pl.when(jnp.logical_not(active))
    def _():
        sent = recv.at[:, pl.ds(0, units)]
        pltpu.make_async_copy(sent, sent, send_sem).wait()
        got = recv.at[0, pl.ds(0, units)]
        pltpu.make_async_copy(got, got, back_recv_sem).wait()

    ret_rows = ret.reshape(BLOCKS, SLOTS, pair, LANES)
    degree = lax.broadcasted_iota(jnp.int32, (pair, degrees), 1)
    degree_sign = jnp.where(lax.rem(degree, 2) == 0, 1.0, -1.0)

    def sum_copy(k):
        return pltpu.make_async_remote_copy(
            src_ref=sum_send.at[k], dst_ref=sum_recv.at[k],
            send_sem=sum_send_sem.at[k], recv_sem=sum_recv_sem.at[k],
            device_id={"lev": partner}, device_id_type=pl.DeviceIdType.MESH,
        )

    @pl.loop(0, SLOTS)
    def _(k):
        mixed = ret_rows[4, k].astype(jnp.float32)
        zero = jnp.zeros_like(mixed)
        tail_north = jnp.where(lane_tile < LANES // 2, mixed, zero).astype(jnp.bfloat16)
        tail_south = jnp.where(lane_tile < LANES // 2, pltpu.roll(mixed, LANES // 2, 1), zero).astype(jnp.bfloat16)
        north = jnp.concatenate([ret_rows[0, k], ret_rows[1, k], tail_north], axis=1)
        south = jnp.concatenate([ret_rows[2, k], ret_rows[3, k], tail_south], axis=1)
        both = jnp.dot(
            jnp.concatenate([north, south], axis=0), basis_ref[k], preferred_element_type=jnp.float32
        )
        combined = both[:pair] + (factors_ref[1, k] * degree_sign) * both[pair:]
        combined = jnp.where(degree >= waves_ref[k], combined, 0.0)
        low, high = combined[:levels], combined[levels:]
        out_ref[k] = jnp.where(x_hi == 0, low, high)
        sum_send[k] = jnp.where(x_hi == 0, high, low).astype(jnp.bfloat16)
        sum_copy(k).start()

    @pl.when(active)
    def _():
        sent = recv.at[0, pl.ds(0, n_lat - 1)]
        pltpu.make_async_copy(sent, sent, back_send_sem).wait()

    @pl.loop(0, SLOTS)
    def _(k):
        copy = sum_copy(k)
        copy.wait()
        out_ref[k] += sum_recv[k].astype(jnp.float32)


def body(n_lat, assign, u_spec, v_spec, basis):
    slots, lev_dev, _, degrees = u_spec.shape
    lev = lax.axis_index("lev")
    x_hi = lev // 2
    core = lev % 2
    levels = 2 * lev_dev
    waves = lax.dynamic_slice_in_dim(assign, lax.axis_index("lat") * slots, slots)

    edge = jnp.where(lev == 2, basis[:, 0], basis[:, -1])
    halo = lax.ppermute(edge, "lev", [(2, 0), (1, 3)]) + lax.ppermute(edge, "lev", [(2, 1), (1, 2)])
    other_basis = lax.ppermute(basis, "lev", PARTNER_CORE)
    other_u = lax.ppermute(u_spec, "lev", PARTNER_X)
    other_v = lax.ppermute(v_spec, "lev", PARTNER_X)

    rows_x = 2 * basis.shape[1]
    low = jnp.where(core == 0, basis, other_basis)
    high = jnp.where(core == 0, other_basis, basis)
    halo_rows = jnp.broadcast_to(halo[:, None], (slots, 64, degrees))
    basis_wide = jnp.concatenate([low, high, halo_rows], axis=1)

    def joined(mine, other):
        first = jnp.where(x_hi == 0, mine, other)
        second = jnp.where(x_hi == 0, other, mine)
        return jnp.concatenate([first, second], axis=1)

    u_all = joined(u_spec, other_u)
    v_all = joined(v_spec, other_v)
    v_turned = jnp.stack([v_all[:, :, 1], -v_all[:, :, 0]], axis=2)
    degree = jnp.arange(degrees, dtype=jnp.int32)
    live = (degree[None, :] >= waves[:, None]).astype(jnp.bfloat16)
    sign = (1 - 2 * ((degree[None, :] + waves[:, None]) % 2)).astype(jnp.bfloat16) * live
    masks = jnp.stack([live, sign], axis=1)[:, None, :, None, :]
    spectra = jnp.stack([u_all, v_turned], axis=1).reshape(slots, 2, 1, 2 * levels, degrees)
    lhs = (spectra * masks).reshape(slots, 8 * levels, degrees)

    angle = waves.astype(jnp.float32) * (2.0 * math.pi / LON)
    factors = jnp.stack([jnp.sin(angle), (1 - 2 * (waves % 2)).astype(jnp.float32)])
    order = jnp.repeat(assign.astype(jnp.float32), 2)
    total = order.shape[0]
    lane_waves = jnp.broadcast_to(order[None, :], (8, total))
    row_waves = jnp.broadcast_to(order[:, None], (total, LANES))

    vmem = pl.BlockSpec(memory_space=pltpu.VMEM)
    smem = pl.BlockSpec(memory_space=pltpu.SMEM)
    result = pl.pallas_call(
        functools.partial(kernel, n_lat, rows_x, levels, degrees),
        out_shape=jax.ShapeDtypeStruct((slots, levels, degrees), jnp.float32),
        in_specs=[smem, smem, vmem, vmem, vmem, vmem],
        out_specs=vmem,
        scratch_shapes=[
            pltpu.VMEM((2, BLOCKS, SLOTS, levels, 2, LANES), jnp.bfloat16),
            pltpu.VMEM((2, n_lat, SLOTS, 2, LANES), jnp.bfloat16),
            pltpu.VMEM((total, 2 * LANES), jnp.bfloat16),
            pltpu.VMEM((LON, LANES), jnp.bfloat16),
            pltpu.VMEM((n_lat, SLOTS, 2, LANES), jnp.bfloat16),
            pltpu.VMEM((BLOCKS, SLOTS, levels, 2, LANES), jnp.bfloat16),
            pltpu.VMEM((SLOTS, levels, degrees), jnp.bfloat16),
            pltpu.VMEM((SLOTS, levels, degrees), jnp.bfloat16),
            pltpu.VMEM((LON, total), jnp.bfloat16),
            pltpu.VMEM((total, LON), jnp.bfloat16),
            pltpu.SemaphoreType.DMA,
            pltpu.SemaphoreType.DMA,
            pltpu.SemaphoreType.DMA,
            pltpu.SemaphoreType.DMA,
            pltpu.SemaphoreType.DMA,
            pltpu.SemaphoreType.DMA,
            pltpu.SemaphoreType.DMA((SLOTS,)),
            pltpu.SemaphoreType.DMA((SLOTS,)),
        ],
        compiler_params=pltpu.CompilerParams(
            collective_id=0, has_side_effects=True, vmem_limit_bytes=48 * 1024 * 1024
        ),
    )(waves, factors, lhs, basis_wide, lane_waves, row_waves)
    return result.reshape(slots, lev_dev, 2, degrees)


def solution(mesh):
    return jax.shard_map(
        functools.partial(body, mesh.shape["lat"]),
        mesh=mesh,
        in_specs=(
            P(),
            P("lat", "lev", None, None),
            P("lat", "lev", None, None),
            P("lat", "lev", None),
        ),
        out_specs=P("lat", "lev", None, None),
        check_vma=False,
    )
```

```python
import functools
import math

import jax
import jax.numpy as jnp
from jax import lax
from jax.experimental import pallas as pl
from jax.experimental.pallas import tpu as pltpu
from jax.sharding import PartitionSpec as P

LON = 2560
SLOTS = 5
BLOCKS = 5
LANES = 128
GROUP = 16
HALF_LEVELS = 8
ROWS = 16


def cos_sin(turns):
    x = turns - jnp.floor(turns + 0.5)
    u = x * x
    cos = jnp.full_like(u, (2 * math.pi) ** 18 / math.factorial(18) * -1.0)
    sin = jnp.full_like(u, (2 * math.pi) ** 19 / math.factorial(19) * -1.0)
    for i in range(8, -1, -1):
        sign = 1.0 if i % 2 == 0 else -1.0
        cos = cos * u + sign * (2 * math.pi) ** (2 * i) / math.factorial(2 * i)
        sin = sin * u + sign * (2 * math.pi) ** (2 * i + 1) / math.factorial(2 * i + 1)
    return cos, sin * x


def tile_rows(value, count):
    return jnp.concatenate([value] * count, axis=0)


def kernel(
    n_lat, half_rows, degrees,
    assign_ref, u_ref, v_ref, basis_ref, lane_waves_ref,
    out_ref,
    wide_basis, u_other, v_other, edge_send, edge_recv,
    send, recv, coeffs, flux, back, ret, sum_send, sum_recv, table_q, table_k, row_waves,
    ready, load_sem, swap_send_sem, swap_recv_sem, edge_send_sem, edge_recv_sem,
    send_sem, recv_sem, local_sem, back_send_sem, back_recv_sem, back_local_sem, sum_send_sem, sum_recv_sem,
):
    me = lax.axis_index("lat")
    lev = lax.axis_index("lev")
    x_hi = lev // 2
    core = lax.rem(lev, 2)
    spread = 2 * lev
    rows_x = 2 * half_rows
    wide = wide_basis.shape[1]
    total = SLOTS * n_lat * 2
    units = BLOCKS * GROUP
    mesh_id = pl.DeviceIdType.MESH

    my_group = me // 8
    my_z = lax.rem(lax.rem(me, 8) + 32 - lax.rem(my_group * 3 + spread, 8), 8)
    my_block = (5 * my_z + 7) // 8
    active = (8 * my_block) // 5 == my_z
    my_level = my_group // 2
    my_half = lax.rem(my_group + my_level, 2)

    def owner_of(block, half, level):
        group = level * 2 + lax.rem(level + half, 2)
        return group * 8 + lax.rem((8 * block) // 5 + lax.rem(group * 3 + spread, 8), 8)

    own_rows = pl.ds(pl.multiple_of(core * half_rows, ROWS), half_rows)
    load = pltpu.make_async_copy(basis_ref, wide_basis.at[:, own_rows], load_sem)
    load.start()

    barrier = pltpu.get_barrier_semaphore()
    for i in range(1, 4):
        pl.semaphore_signal(barrier, inc=1, device_id={"lev": lax.rem(lev + i, 4)}, device_id_type=mesh_id)
    plane = me - lax.rem(me, GROUP)

    @pl.loop(1, GROUP)
    def _(i):
        peer = plane + lax.rem(me + i, GROUP)
        pl.semaphore_signal(barrier, inc=1, device_id={"lat": peer}, device_id_type=mesh_id)

    planes = n_lat // GROUP

    @pl.loop(1, planes)
    def _(i):
        peer = lax.rem(me + i * GROUP, n_lat)
        pl.semaphore_signal(barrier, inc=1, device_id={"lat": peer}, device_id_type=mesh_id)

    pl.semaphore_wait(barrier, 3 + GROUP - 1 + planes - 1)

    partner = lax.rem(lev + 2, 4)
    sibling = 2 * x_hi + 1 - core

    def swap(i, source, target, device):
        return pltpu.make_async_remote_copy(
            src_ref=source, dst_ref=target, send_sem=swap_send_sem.at[i], recv_sem=swap_recv_sem.at[i],
            device_id={"lev": device}, device_id_type=mesh_id,
        )

    swap_u = swap(0, u_ref, u_other, partner)
    swap_v = swap(1, v_ref, v_other, partner)
    swap_u.start()
    swap_v.start()

    @pl.loop(1, planes)
    def _(i):
        peer = lax.rem(me + i * GROUP, n_lat)
        pl.semaphore_signal(ready, inc=1, device_id={"lat": peer}, device_id_type=mesh_id)

    load.wait()
    swap_basis = swap(2, wide_basis.at[:, own_rows], wide_basis.at[:, own_rows], sibling)
    swap_basis.start()

    inner = x_hi + core == 1
    edge_base = 2 - 2 * x_hi

    def edge_copy(i):
        return pltpu.make_async_remote_copy(
            src_ref=edge_send, dst_ref=edge_recv, send_sem=edge_send_sem.at[i], recv_sem=edge_recv_sem,
            device_id={"lev": edge_base + i}, device_id_type=mesh_id,
        )

    @pl.when(inner & (x_hi == 1))
    def _():
        for k in range(SLOTS):
            edge_send[k] = jnp.broadcast_to(wide_basis[k, 0:ROWS, :][0:1], (2, degrees))

    @pl.when(inner & (x_hi == 0))
    def _():
        for k in range(SLOTS):
            edge_send[k] = jnp.broadcast_to(wide_basis[k, rows_x - ROWS : rows_x, :][ROWS - 1 :], (2, degrees))

    @pl.when(inner)
    def _():
        edge_copy(0).start()
        edge_copy(1).start()

    for t in range(total // LANES):
        square = jnp.broadcast_to(lane_waves_ref[0:1, t * LANES : (t + 1) * LANES], (LANES, LANES))
        row_waves[t * LANES : (t + 1) * LANES, :] = square.T

    edge_copy(0).wait_recv()
    for k in range(SLOTS):
        wide_basis[k, rows_x:wide, :] = jnp.broadcast_to(edge_recv[k][0:1], (wide - rows_x, degrees))
    swap_basis.wait()

    send_rows = send.reshape(2, BLOCKS, SLOTS, 2, ROWS, LANES)
    lane = lax.broadcasted_iota(jnp.int32, (2 * ROWS, wide), 1)
    row = lax.broadcasted_iota(jnp.int32, (2 * ROWS, wide), 0)
    half_sign = jnp.where(row < ROWS, -0.5, 0.5)
    even = lax.rem(row, 2) == 0
    lane_tile = lax.broadcasted_iota(jnp.int32, (ROWS, LANES), 1)
    degree = lax.broadcasted_iota(jnp.int32, (8, degrees), 1)
    degree_sign = (1 - 2 * lax.rem(degree, 2)).astype(jnp.float32)

    def factors(k):
        wave = assign_ref[me * SLOTS + k]
        parity = (1 - 2 * lax.rem(wave, 2)).astype(jnp.float32)
        live = jnp.where(degree >= wave, 1.0, 0.0)
        return wave, parity, live, live * (parity * degree_sign)

    def meridional(half, u_rows, v_rows):
        @pl.loop(0, SLOTS)
        def _(k):
            wave, parity, live, signed = factors(k)
            live = tile_rows(live, 2).astype(jnp.bfloat16)
            signed = tile_rows(signed, 2).astype(jnp.bfloat16)
            u, v = u_rows[k], v_rows[k]
            lhs = jnp.concatenate([u * live, u * signed, v * live, v * signed], axis=0)
            fields = lax.dot_general(
                lhs, wide_basis[k], (((1,), (1,)), ((), ())), preferred_element_type=jnp.float32
            )
            wind, other = fields[: 2 * ROWS], fields[2 * ROWS :]
            turned = jnp.where(even, pltpu.roll(other, 2 * ROWS - 1, 0), -pltpu.roll(other, 1, 0))
            sine = cos_sin(jnp.full((8, wide), 1.0 / LON, jnp.float32) * wave.astype(jnp.float32))[1]
            before = pltpu.roll(wind, 1, 1)
            after = pltpu.roll(wind, wide - 1, 1)
            swapped = jnp.concatenate([wind[ROWS:], wind[:ROWS]], axis=0)
            before = jnp.where((lane == 0) & (x_hi == 0), -parity * wind, before)
            after = jnp.where((lane == rows_x - 1) & (x_hi == 1), swapped, after)
            curl = tile_rows(sine, 2 * ROWS // 8) * turned + half_sign * (before - after)
            for f, value in enumerate((wind, curl)):
                north, south = value[:ROWS], value[ROWS:]
                tail = 2 * LANES
                mixed = jnp.where(
                    lane_tile < LANES // 2,
                    north[:, tail : tail + LANES],
                    pltpu.roll(south[:, tail : tail + LANES], LANES // 2, 1),
                )
                tiles = (north[:, :LANES], north[:, LANES:tail], south[:, :LANES], south[:, LANES:tail], mixed)
                for b, tile in enumerate(tiles):
                    send_rows[f, b, k, half] = tile.astype(jnp.bfloat16)

        @pl.loop(0, units // 2)
        def _(i):
            block = lax.rem(i, BLOCKS)
            level = lax.rem(i // BLOCKS + my_level, HALF_LEVELS)
            source = send.at[:, block, :, half, level]
            owner = owner_of(block, half, level)

            @pl.when(owner != me)
            def _():
                pltpu.make_async_remote_copy(
                    src_ref=source, dst_ref=recv.at[:, me], send_sem=send_sem, recv_sem=recv_sem,
                    device_id={"lat": owner}, device_id_type=mesh_id,
                ).start()

            @pl.when(owner == me)
            def _():
                pltpu.make_async_copy(source, recv.at[:, me], local_sem).start()

    pl.semaphore_wait(ready, planes - 1)
    meridional(0, u_ref.reshape(SLOTS, ROWS, degrees), v_ref.reshape(SLOTS, ROWS, degrees))

    chunk = 64

    @pl.loop(0, total // chunk)
    def _(i):
        rows = pl.ds(pl.multiple_of(i * chunk, chunk), chunk)
        wave = row_waves[rows, :]
        column = lax.broadcasted_iota(jnp.int32, (chunk, LANES), 1).astype(jnp.float32)
        part = lax.broadcasted_iota(jnp.int32, (chunk, LANES), 0)
        shift = lax.rem(part, 2).astype(jnp.float32) * 0.25
        cos, sin = cos_sin(wave * column * (1.0 / LON) - shift)
        turn_cos, turn_sin = cos_sin(wave * (LANES / LON))
        for step in range(LON // LANES):
            table_k[rows, step * LANES : (step + 1) * LANES] = cos.astype(jnp.bfloat16)
            cos, sin = cos * turn_cos - sin * turn_sin, sin * turn_cos + cos * turn_sin

    swap_u.wait()
    swap_v.wait()
    meridional(1, u_other.reshape(SLOTS, ROWS, degrees), v_other.reshape(SLOTS, ROWS, degrees))

    width = total // 2
    for part in range(2):
        lanes = pl.ds(part * width, width)
        height = 16
        wave = jnp.broadcast_to(lane_waves_ref[0:1, lanes], (height, width))
        position = lax.broadcasted_iota(jnp.int32, (height, width), 0).astype(jnp.float32)
        side = lax.broadcasted_iota(jnp.int32, (height, width), 1)
        shift = lax.rem(side, 2).astype(jnp.float32) * 0.25
        start = cos_sin(wave * position * (1.0 / LON) - shift)
        turn_cos, turn_sin = cos_sin(lane_waves_ref[0:8, lanes] * (height / LON))
        turn_cos, turn_sin = tile_rows(turn_cos, 2), tile_rows(turn_sin, 2)

        def advance(i, carry):
            cos, sin = carry
            table_q[pl.ds(pl.multiple_of(i * height, height), height), lanes] = cos.astype(jnp.bfloat16)
            return cos * turn_cos - sin * turn_sin, sin * turn_cos + cos * turn_sin

        lax.fori_loop(0, LON // height, advance, start)

    @pl.when(inner)
    def _():
        edge_copy(0).wait_send()
        edge_copy(1).wait_send()

    @pl.when(active)
    def _():
        remote = recv.at[:, pl.ds(0, n_lat - 1)]
        pltpu.make_async_copy(remote, remote, recv_sem).wait()
        pltpu.make_async_copy(recv.at[:, 0], recv.at[:, 0], local_sem).wait()
        recv_rows = recv.reshape(2, total, LANES)
        coeffs[:, :LANES] = recv_rows[0]
        coeffs[:, LANES:] = recv_rows[1]
        step = 256

        @pl.loop(0, LON // step)
        def _(i):
            rows = pl.ds(pl.multiple_of(i * step, step), step)
            grid = jnp.dot(table_q[rows, :], coeffs[...], preferred_element_type=jnp.float32)
            flux[rows, :] = (grid[:, :LANES] * grid[:, LANES:]).astype(jnp.bfloat16)

        back_rows = back.reshape(total, LANES)
        pieces = 4
        owners = n_lat // pieces
        high = total // pieces

        @pl.loop(0, pieces)
        def _(i):
            piece = lax.rem(i + me // owners, pieces)
            rows = pl.ds(pl.multiple_of(piece * high, high), high)
            zonal = jnp.dot(table_k[rows, :], flux[...], preferred_element_type=jnp.float32)
            back_rows[rows, :] = (zonal * (1.0 / math.sqrt(LON))).astype(jnp.bfloat16)

            @pl.loop(0, owners)
            def _(j):
                owner = piece * owners + lax.rem(j + me, owners)
                target = ret.at[my_block, :, my_half, my_level]

                @pl.when(owner != me)
                def _():
                    pltpu.make_async_remote_copy(
                        src_ref=back.at[owner], dst_ref=target, send_sem=back_send_sem, recv_sem=back_recv_sem,
                        device_id={"lat": owner}, device_id_type=mesh_id,
                    ).start()

                @pl.when(owner == me)
                def _():
                    pltpu.make_async_copy(back.at[owner], target, back_local_sem).start()

        pltpu.make_async_copy(back.at[me], back.at[me], back_local_sem).wait()
        sent = recv.at[:, pl.ds(0, units - 1)]
        pltpu.make_async_copy(sent, sent, send_sem).wait()
        got = recv.at[0, pl.ds(0, units - 1)]
        pltpu.make_async_copy(got, got, back_recv_sem).wait()

    @pl.when(jnp.logical_not(active))
    def _():
        sent = recv.at[:, pl.ds(0, units)]
        pltpu.make_async_copy(sent, sent, send_sem).wait()
        got = recv.at[0, pl.ds(0, units)]
        pltpu.make_async_copy(got, got, back_recv_sem).wait()

    ret_rows = ret.reshape(BLOCKS, SLOTS, 2 * ROWS, LANES)
    wide_lane = lax.broadcasted_iota(jnp.int32, (2 * ROWS, LANES), 1)

    def sum_copy(k):
        return pltpu.make_async_remote_copy(
            src_ref=sum_send.at[k], dst_ref=sum_recv.at[k],
            send_sem=sum_send_sem.at[k], recv_sem=sum_recv_sem.at[k],
            device_id={"lev": partner}, device_id_type=mesh_id,
        )

    @pl.loop(0, SLOTS)
    def _(k):
        wave, parity, live, signed = factors(k)
        mixed = ret_rows[4, k].astype(jnp.float32)
        zero = jnp.zeros_like(mixed)
        tail_north = jnp.where(wide_lane < LANES // 2, mixed, zero).astype(jnp.bfloat16)
        tail_south = jnp.where(wide_lane < LANES // 2, pltpu.roll(mixed, LANES // 2, 1), zero).astype(jnp.bfloat16)
        north = jnp.concatenate([ret_rows[0, k], ret_rows[1, k], tail_north], axis=1)
        south = jnp.concatenate([ret_rows[2, k], ret_rows[3, k], tail_south], axis=1)
        both = jnp.dot(
            jnp.concatenate([north, south], axis=0), wide_basis[k], preferred_element_type=jnp.float32
        )
        combined = tile_rows(live, 4) * both[: 2 * ROWS] + tile_rows(signed, 4) * both[2 * ROWS :]
        sum_send[k] = combined[ROWS:].astype(jnp.bfloat16)
        sum_copy(k).start()
        out_ref[k] = combined[:ROWS]

    @pl.when(active)
    def _():
        sent = recv.at[0, pl.ds(0, n_lat - 1)]
        pltpu.make_async_copy(sent, sent, back_send_sem).wait()

    @pl.loop(0, SLOTS)
    def _(k):
        sum_copy(k).wait()
        out_ref[k] += sum_recv[k].astype(jnp.float32)


def body(n_lat, assign, u_spec, v_spec, basis):
    slots, lev_dev, _, degrees = u_spec.shape
    half_rows = basis.shape[1]
    order = jnp.repeat(assign.astype(jnp.float32), 2)
    total = order.shape[0]
    lane_waves = jnp.broadcast_to(order[None, :], (8, total))
    wide = 3 * LANES

    vmem = pl.BlockSpec(memory_space=pltpu.VMEM)
    smem = pl.BlockSpec(memory_space=pltpu.SMEM)
    bf16 = jnp.bfloat16
    dma = pltpu.SemaphoreType.DMA
    result = pl.pallas_call(
        functools.partial(kernel, n_lat, half_rows, degrees),
        out_shape=jax.ShapeDtypeStruct((slots, ROWS, degrees), jnp.float32),
        in_specs=[smem, vmem, vmem, pl.BlockSpec(memory_space=pl.ANY), vmem],
        out_specs=vmem,
        scratch_shapes=[
            pltpu.VMEM((slots, wide, degrees), bf16),
            pltpu.VMEM((slots, lev_dev, 2, degrees), bf16),
            pltpu.VMEM((slots, lev_dev, 2, degrees), bf16),
            pltpu.VMEM((slots, 2, degrees), bf16),
            pltpu.VMEM((slots, 2, degrees), bf16),
            pltpu.VMEM((2, BLOCKS, SLOTS, 2, HALF_LEVELS, 2, LANES), bf16),
            pltpu.VMEM((2, n_lat, SLOTS, 2, LANES), bf16),
            pltpu.VMEM((total, 2 * LANES), bf16),
            pltpu.VMEM((LON, LANES), bf16),
            pltpu.VMEM((n_lat, SLOTS, 2, LANES), bf16),
            pltpu.VMEM((BLOCKS, SLOTS, 2, HALF_LEVELS, 2, LANES), bf16),
            pltpu.VMEM((SLOTS, ROWS, degrees), bf16),
            pltpu.VMEM((SLOTS, ROWS, degrees), bf16),
            pltpu.VMEM((LON, total), bf16),
            pltpu.VMEM((total, LON), bf16),
            pltpu.VMEM((total, LANES), jnp.float32),
            pltpu.SemaphoreType.REGULAR,
            dma, dma((3,)), dma((3,)), dma((2,)), dma,
            dma, dma, dma, dma, dma, dma, dma((SLOTS,)), dma((SLOTS,)),
        ],
        compiler_params=pltpu.CompilerParams(
            collective_id=0, has_side_effects=True, vmem_limit_bytes=48 * 1024 * 1024
        ),
    )(assign, u_spec, v_spec, basis, lane_waves)
    return result.reshape(slots, lev_dev, 2, degrees)


def solution(mesh):
    return jax.shard_map(
        functools.partial(body, mesh.shape["lat"]),
        mesh=mesh,
        in_specs=(
            P(),
            P("lat", "lev", None, None),
            P("lat", "lev", None, None),
            P("lat", "lev", None),
        ),
        out_specs=P("lat", "lev", None, None),
        check_vma=False,
    )
```

```python
import functools
import math

import jax
import jax.numpy as jnp
from jax import lax
from jax.experimental import pallas as pl
from jax.experimental.pallas import tpu as pltpu
from jax.sharding import PartitionSpec as P

LON = 2560
SLOTS = 5
BLOCKS = 5
LANES = 128
GROUP = 16
HALF_LEVELS = 8
ROWS = 16


def cos_sin(turns):
    x = turns - jnp.floor(turns + 0.5)
    u = x * x
    cos = jnp.full_like(u, (2 * math.pi) ** 18 / math.factorial(18) * -1.0)
    sin = jnp.full_like(u, (2 * math.pi) ** 19 / math.factorial(19) * -1.0)
    for i in range(8, -1, -1):
        sign = 1.0 if i % 2 == 0 else -1.0
        cos = cos * u + sign * (2 * math.pi) ** (2 * i) / math.factorial(2 * i)
        sin = sin * u + sign * (2 * math.pi) ** (2 * i + 1) / math.factorial(2 * i + 1)
    return cos, sin * x


def tile_rows(value, count):
    return jnp.concatenate([value] * count, axis=0)


def parity_of(wave):
    return 1.0 - 2.0 * (wave - 2.0 * jnp.floor(0.5 * wave))


def kernel(
    n_lat, half_rows, degrees,
    assign_ref, assign_lanes_ref, u_ref, v_ref, basis_ref,
    out_ref,
    wide_basis, u_own, v_own, u_other, v_other, edge_send, edge_recv,
    send, recv, split, cos_coeffs, sin_coeffs, cos_flux, sin_flux, mix, back, ret, sum_send, sum_recv,
    cos_q, sin_q, end_q, cos_k, sin_k, row_waves,
    ready, load_sem, swap_send_sem, swap_recv_sem, edge_send_sem, edge_recv_sem,
    send_sem, recv_sem, local_sem, back_send_sem, back_recv_sem, back_local_sem, sum_send_sem, sum_recv_sem,
):
    me = lax.axis_index("lat")
    lev = lax.axis_index("lev")
    x_hi = lev // 2
    core = lax.rem(lev, 2)
    spread = 2 * lev
    rows_x = 2 * half_rows
    wide = wide_basis.shape[1]
    waves = SLOTS * n_lat
    half_lon = LON // 2
    units = BLOCKS * GROUP
    mesh_id = pl.DeviceIdType.MESH

    my_group = me // 8
    my_z = lax.rem(lax.rem(me, 8) + 32 - lax.rem(my_group * 3 + spread, 8), 8)
    my_block = (5 * my_z + 7) // 8
    active = (8 * my_block) // 5 == my_z
    my_level = my_group // 2
    my_half = lax.rem(my_group + my_level, 2)

    own_rows = pl.ds(pl.multiple_of(core * half_rows, ROWS), half_rows)
    loads = [
        pltpu.make_async_copy(basis_ref, wide_basis.at[:, own_rows], load_sem.at[0]),
        pltpu.make_async_copy(u_ref, u_own, load_sem.at[1]),
        pltpu.make_async_copy(v_ref, v_own, load_sem.at[2]),
    ]
    for load in loads:
        load.start()

    barrier = pltpu.get_barrier_semaphore()
    for i in range(1, 4):
        pl.semaphore_signal(barrier, inc=1, device_id={"lev": lax.rem(lev + i, 4)}, device_id_type=mesh_id)
    plane = me - lax.rem(me, GROUP)

    @pl.loop(1, GROUP)
    def _(i):
        peer = plane + lax.rem(me + i, GROUP)
        pl.semaphore_signal(barrier, inc=1, device_id={"lat": peer}, device_id_type=mesh_id)

    planes = n_lat // GROUP

    @pl.loop(1, planes)
    def _(i):
        peer = lax.rem(me + i * GROUP, n_lat)
        pl.semaphore_signal(barrier, inc=1, device_id={"lat": peer}, device_id_type=mesh_id)

    pl.semaphore_wait(barrier, 3 + GROUP - 1 + planes - 1)

    partner = lax.rem(lev + 2, 4)
    sibling = 2 * x_hi + 1 - core

    def swap(i, source, target, device):
        return pltpu.make_async_remote_copy(
            src_ref=source, dst_ref=target, send_sem=swap_send_sem.at[i], recv_sem=swap_recv_sem.at[i],
            device_id={"lev": device}, device_id_type=mesh_id,
        )

    swap_u = swap(0, u_own, u_other, partner)
    swap_v = swap(1, v_own, v_other, partner)
    swap_basis = swap(2, wide_basis.at[:, own_rows], wide_basis.at[:, own_rows], sibling)

    @pl.loop(1, planes)
    def _(i):
        peer = lax.rem(me + i * GROUP, n_lat)
        pl.semaphore_signal(ready, inc=1, device_id={"lat": peer}, device_id_type=mesh_id)

    loads[0].wait()
    swap_basis.start()

    inner = x_hi + core == 1
    edge_base = 2 - 2 * x_hi

    def edge_copy(i):
        return pltpu.make_async_remote_copy(
            src_ref=edge_send, dst_ref=edge_recv, send_sem=edge_send_sem.at[i], recv_sem=edge_recv_sem,
            device_id={"lev": edge_base + i}, device_id_type=mesh_id,
        )

    @pl.when(inner & (x_hi == 1))
    def _():
        for k in range(SLOTS):
            edge_send[k] = jnp.broadcast_to(wide_basis[k, 0:ROWS, :][0:1], (2, degrees))

    @pl.when(inner & (x_hi == 0))
    def _():
        for k in range(SLOTS):
            edge_send[k] = jnp.broadcast_to(wide_basis[k, rows_x - ROWS : rows_x, :][ROWS - 1 :], (2, degrees))

    @pl.when(inner)
    def _():
        edge_copy(0).start()
        edge_copy(1).start()

    loads[1].wait()
    swap_u.start()
    loads[2].wait()
    swap_v.start()

    lane_waves = []
    for t in range(waves // LANES):
        line = assign_lanes_ref[t : t + 1, :].astype(jnp.float32)
        lane_waves.append(jnp.broadcast_to(line, (8, LANES)))
        row_waves[t * LANES : (t + 1) * LANES, :] = jnp.broadcast_to(line, (LANES, LANES)).T

    chunk = 64

    @pl.loop(0, waves // chunk)
    def _(i):
        rows = pl.ds(pl.multiple_of(i * chunk, chunk), chunk)
        wave = row_waves[rows, :]
        column = lax.broadcasted_iota(jnp.int32, (chunk, LANES), 1).astype(jnp.float32)
        cos, sin = cos_sin(wave * column * (1.0 / LON))
        turn_cos, turn_sin = cos_sin(wave * (LANES / LON))
        for step in range(half_lon // LANES):
            lanes = slice(step * LANES, (step + 1) * LANES)
            cos_k[rows, lanes] = cos.astype(jnp.bfloat16)
            sin_k[rows, lanes] = sin.astype(jnp.bfloat16)
            cos, sin = cos * turn_cos - sin * turn_sin, sin * turn_cos + cos * turn_sin

    edge_copy(0).wait_recv()
    for k in range(SLOTS):
        wide_basis[k, rows_x:wide, :] = jnp.broadcast_to(edge_recv[k][0:1], (wide - rows_x, degrees))
    swap_basis.wait()

    send_rows = send.reshape(2, BLOCKS, SLOTS, 2, ROWS, LANES)
    lane = lax.broadcasted_iota(jnp.int32, (2 * ROWS, wide), 1)
    row = lax.broadcasted_iota(jnp.int32, (2 * ROWS, wide), 0)
    half_sign = jnp.where(row < ROWS, -0.5, 0.5)
    even = lax.rem(row, 2) == 0
    lane_tile = lax.broadcasted_iota(jnp.int32, (ROWS, LANES), 1)
    degree = lax.broadcasted_iota(jnp.int32, (8, degrees), 1)
    degree_sign = (1 - 2 * lax.rem(degree, 2)).astype(jnp.float32)

    def factors(k):
        wave = assign_ref[me * SLOTS + k]
        parity = (1 - 2 * lax.rem(wave, 2)).astype(jnp.float32)
        live = jnp.where(degree >= wave, 1.0, 0.0)
        return wave, parity, live, live * (parity * degree_sign)

    def meridional(half, u_rows, v_rows):
        for k in range(SLOTS):
            wave, parity, live, signed = factors(k)
            live = tile_rows(live, 2).astype(jnp.bfloat16)
            signed = tile_rows(signed, 2).astype(jnp.bfloat16)
            u, v = u_rows[k], v_rows[k]
            lhs = jnp.concatenate([u * live, u * signed, v * live, v * signed], axis=0)
            fields = lax.dot_general(
                wide_basis[k], lhs, (((1,), (1,)), ((), ())), preferred_element_type=jnp.float32
            ).T
            wind, other = fields[: 2 * ROWS], fields[2 * ROWS :]
            turned = jnp.where(even, pltpu.roll(other, 2 * ROWS - 1, 0), -pltpu.roll(other, 1, 0))
            sine = cos_sin(jnp.full((8, wide), 1.0 / LON, jnp.float32) * wave.astype(jnp.float32))[1]
            before = pltpu.roll(wind, 1, 1)
            after = pltpu.roll(wind, wide - 1, 1)
            swapped = jnp.concatenate([wind[ROWS:], wind[:ROWS]], axis=0)
            before = jnp.where((lane == 0) & (x_hi == 0), -parity * wind, before)
            after = jnp.where((lane == rows_x - 1) & (x_hi == 1), swapped, after)
            curl = tile_rows(sine, 2 * ROWS // 8) * turned + half_sign * (before - after)
            for f, value in enumerate((wind, curl)):
                north, south = value[:ROWS], value[ROWS:]
                tail = 2 * LANES
                mixed = jnp.where(
                    lane_tile < LANES // 2,
                    north[:, tail : tail + LANES],
                    pltpu.roll(south[:, tail : tail + LANES], LANES // 2, 1),
                )
                tiles = (north[:, :LANES], north[:, LANES:tail], south[:, :LANES], south[:, LANES:tail], mixed)
                for b, tile in enumerate(tiles):
                    send_rows[f, b, k, half] = tile.astype(jnp.bfloat16)

        def send_unit(block, group, level, turn):
            owner = group * 8 + lax.rem((8 * block) // 5 + turn, 8)
            return owner, pltpu.make_async_remote_copy(
                src_ref=send.at[:, block, :, half, level], dst_ref=recv.at[:, me], send_sem=send_sem, recv_sem=recv_sem,
                device_id={"lat": owner}, device_id_type=mesh_id,
            )

        def place(level):
            group = level * 2 + lax.rem(level + half, 2)
            return group, lax.rem(group * 3 + spread, 8)

        group, turn = place(my_level)
        for block in range(BLOCKS):
            owner, copy = send_unit(block, group, my_level, turn)

            @pl.when(owner != me)
            def _():
                copy.start()

            @pl.when(owner == me)
            def _():
                pltpu.make_async_copy(send.at[:, block, :, half, my_level], recv.at[:, me], local_sem).start()

        for i in range(1, HALF_LEVELS):
            level = lax.rem(my_level + i, HALF_LEVELS)
            group, turn = place(level)
            for block in range(BLOCKS):
                send_unit(block, group, level, turn)[1].start()

    pl.semaphore_wait(ready, planes - 1)
    meridional(0, u_own.reshape(SLOTS, ROWS, degrees), v_own.reshape(SLOTS, ROWS, degrees))

    swap_u.wait()
    swap_v.wait()
    meridional(1, u_other.reshape(SLOTS, ROWS, degrees), v_other.reshape(SLOTS, ROWS, degrees))

    wave = jnp.concatenate(lane_waves, axis=1)
    end_q[...] = tile_rows(parity_of(wave), ROWS // 8).astype(jnp.bfloat16)
    turn_cos, turn_sin = cos_sin(wave * (ROWS / LON))
    turn_cos, turn_sin = tile_rows(turn_cos, ROWS // 8), tile_rows(turn_sin, ROWS // 8)
    position = lax.broadcasted_iota(jnp.int32, (ROWS, waves), 0).astype(jnp.float32)

    def advance(i, carry):
        cos, sin = carry
        rows = pl.ds(pl.multiple_of(i * ROWS, ROWS), ROWS)
        cos_q[rows, :] = cos.astype(jnp.bfloat16)
        sin_q[rows, :] = sin.astype(jnp.bfloat16)
        return cos * turn_cos - sin * turn_sin, sin * turn_cos + cos * turn_sin

    lax.fori_loop(0, half_lon // ROWS, advance, cos_sin(tile_rows(wave, ROWS // 8) * position * (1.0 / LON)))

    @pl.when(inner)
    def _():
        edge_copy(0).wait_send()
        edge_copy(1).wait_send()

    @pl.when(active)
    def _():
        remote = recv.at[:, pl.ds(0, n_lat - 1)]
        pltpu.make_async_copy(remote, remote, recv_sem).wait()
        pltpu.make_async_copy(recv.at[:, 0], recv.at[:, 0], local_sem).wait()
        recv_rows = recv.reshape(2, 2 * waves, LANES)
        for f in range(2):
            lanes = slice(f * LANES, (f + 1) * LANES)
            split[f] = recv_rows[f].astype(jnp.float32)
            cos_coeffs[:, lanes] = split[f, pl.ds(0, waves, 2), :].astype(jnp.bfloat16)
            sin_coeffs[:, lanes] = split[f, pl.ds(1, waves, 2), :].astype(jnp.bfloat16)
        step = 256
        first_row = lax.broadcasted_iota(jnp.int32, (step, LANES), 0)

        @pl.loop(0, half_lon // step)
        def _(i):
            rows = pl.ds(pl.multiple_of(i * step, step), step)
            cos = jnp.dot(cos_q[rows, :], cos_coeffs[...], preferred_element_type=jnp.float32)
            sin = jnp.dot(sin_q[rows, :], sin_coeffs[...], preferred_element_type=jnp.float32)
            cos_u, cos_w = cos[:, :LANES], cos[:, LANES:]
            sin_u, sin_w = sin[:, :LANES], sin[:, LANES:]
            share = jnp.where(first_row + i * step == 0, 0.5, 1.0)
            cos_flux[rows, :] = (share * (cos_u * cos_w + sin_u * sin_w)).astype(jnp.bfloat16)
            sin_flux[rows, :] = (cos_u * sin_w + sin_u * cos_w).astype(jnp.bfloat16)

        end = jnp.dot(end_q[...], cos_coeffs[...], preferred_element_type=jnp.float32)
        end_flux = 0.5 * end[0:1, :LANES] * end[0:1, LANES:]

        back_rows = back.reshape(2 * waves, LANES)
        pieces = 4
        owners = n_lat // pieces
        high = waves // pieces
        scale = 2.0 / math.sqrt(LON)

        target = ret.at[my_block, :, my_half, my_level]
        my_piece = me // owners
        my_place = lax.rem(me, owners)
        for i in range(pieces):
            piece = lax.rem(my_piece + 1 + i, pieces)
            rows = pl.ds(pl.multiple_of(piece * high, high), high)
            cos = jnp.dot(cos_k[rows, :], cos_flux[...], preferred_element_type=jnp.float32)
            sin = jnp.dot(sin_k[rows, :], sin_flux[...], preferred_element_type=jnp.float32)
            cos = cos + parity_of(row_waves[rows, :]) * end_flux
            mix[i, pl.ds(0, high, 2), :] = cos * scale
            mix[i, pl.ds(1, high, 2), :] = sin * scale
            both = pl.ds(pl.multiple_of(piece * 2 * high, 2 * high), 2 * high)
            back_rows[both, :] = mix[i].astype(jnp.bfloat16)
            if i == pieces - 1:
                pltpu.make_async_copy(back.at[me], target, back_local_sem).start()
            for j in range(1 if i == pieces - 1 else 0, owners):
                owner = piece * owners + lax.rem(my_place + j, owners)
                pltpu.make_async_remote_copy(
                    src_ref=back.at[owner], dst_ref=target, send_sem=back_send_sem, recv_sem=back_recv_sem,
                    device_id={"lat": owner}, device_id_type=mesh_id,
                ).start()

        pltpu.make_async_copy(back.at[me], back.at[me], back_local_sem).wait()
        sent = recv.at[:, pl.ds(0, units - 1)]
        pltpu.make_async_copy(sent, sent, send_sem).wait()
        got = recv.at[0, pl.ds(0, units - 1)]
        pltpu.make_async_copy(got, got, back_recv_sem).wait()

    @pl.when(jnp.logical_not(active))
    def _():
        sent = recv.at[:, pl.ds(0, units)]
        pltpu.make_async_copy(sent, sent, send_sem).wait()
        got = recv.at[0, pl.ds(0, units)]
        pltpu.make_async_copy(got, got, back_recv_sem).wait()

    ret_rows = ret.reshape(BLOCKS, SLOTS, 2 * ROWS, LANES)
    wide_lane = lax.broadcasted_iota(jnp.int32, (2 * ROWS, LANES), 1)

    def sum_copy(k):
        return pltpu.make_async_remote_copy(
            src_ref=sum_send.at[k], dst_ref=sum_recv.at[k],
            send_sem=sum_send_sem.at[k], recv_sem=sum_recv_sem.at[k],
            device_id={"lev": partner}, device_id_type=mesh_id,
        )

    for k in range(SLOTS):
        wave, parity, live, signed = factors(k)
        mixed = ret_rows[4, k].astype(jnp.float32)
        zero = jnp.zeros_like(mixed)
        tail_north = jnp.where(wide_lane < LANES // 2, mixed, zero).astype(jnp.bfloat16)
        tail_south = jnp.where(wide_lane < LANES // 2, pltpu.roll(mixed, LANES // 2, 1), zero).astype(jnp.bfloat16)
        north = jnp.concatenate([ret_rows[0, k], ret_rows[1, k], tail_north], axis=1)
        south = jnp.concatenate([ret_rows[2, k], ret_rows[3, k], tail_south], axis=1)
        both = jnp.dot(
            jnp.concatenate([north, south], axis=0), wide_basis[k], preferred_element_type=jnp.float32
        )
        combined = tile_rows(live, 4) * both[: 2 * ROWS] + tile_rows(signed, 4) * both[2 * ROWS :]
        sum_send[k] = combined[ROWS:].astype(jnp.bfloat16)
        sum_copy(k).start()
        out_ref[k] = combined[:ROWS]

    @pl.when(active)
    def _():
        sent = recv.at[0, pl.ds(0, n_lat - 1)]
        pltpu.make_async_copy(sent, sent, back_send_sem).wait()

    @pl.loop(0, SLOTS)
    def _(k):
        sum_copy(k).wait()
        out_ref[k] += sum_recv[k].astype(jnp.float32)


def body(n_lat, assign, u_spec, v_spec, basis):
    slots, lev_dev, _, degrees = u_spec.shape
    half_rows = basis.shape[1]
    waves = assign.shape[0]
    wide = 3 * LANES

    vmem = pl.BlockSpec(memory_space=pltpu.VMEM)
    smem = pl.BlockSpec(memory_space=pltpu.SMEM)
    hbm = pl.BlockSpec(memory_space=pltpu.HBM)
    bf16 = jnp.bfloat16
    f32 = jnp.float32
    dma = pltpu.SemaphoreType.DMA
    result = pl.pallas_call(
        functools.partial(kernel, n_lat, half_rows, degrees),
        out_shape=jax.ShapeDtypeStruct((slots, ROWS, degrees), jnp.float32),
        in_specs=[smem, vmem, hbm, hbm, hbm],
        out_specs=vmem,
        scratch_shapes=[
            pltpu.VMEM((slots, wide, degrees), bf16),
            pltpu.VMEM((slots, lev_dev, 2, degrees), bf16),
            pltpu.VMEM((slots, lev_dev, 2, degrees), bf16),
            pltpu.VMEM((slots, lev_dev, 2, degrees), bf16),
            pltpu.VMEM((slots, lev_dev, 2, degrees), bf16),
            pltpu.VMEM((slots, 2, degrees), bf16),
            pltpu.VMEM((slots, 2, degrees), bf16),
            pltpu.VMEM((2, BLOCKS, SLOTS, 2, HALF_LEVELS, 2, LANES), bf16),
            pltpu.VMEM((2, n_lat, SLOTS, 2, LANES), bf16),
            pltpu.VMEM((2, 2 * waves, LANES), f32),
            pltpu.VMEM((waves, 2 * LANES), bf16),
            pltpu.VMEM((waves, 2 * LANES), bf16),
            pltpu.VMEM((LON // 2, LANES), bf16),
            pltpu.VMEM((LON // 2, LANES), bf16),
            pltpu.VMEM((4, waves // 2, LANES), f32),
            pltpu.VMEM((n_lat, SLOTS, 2, LANES), bf16),
            pltpu.VMEM((BLOCKS, SLOTS, 2, HALF_LEVELS, 2, LANES), bf16),
            pltpu.VMEM((SLOTS, ROWS, degrees), bf16),
            pltpu.VMEM((SLOTS, ROWS, degrees), bf16),
            pltpu.VMEM((LON // 2, waves), bf16),
            pltpu.VMEM((LON // 2, waves), bf16),
            pltpu.VMEM((ROWS, waves), bf16),
            pltpu.VMEM((waves, LON // 2), bf16),
            pltpu.VMEM((waves, LON // 2), bf16),
            pltpu.VMEM((waves, LANES), f32),
            pltpu.SemaphoreType.REGULAR,
            dma((3,)), dma((3,)), dma((3,)), dma((2,)), dma,
            dma, dma, dma, dma, dma, dma, dma((SLOTS,)), dma((SLOTS,)),
        ],
        compiler_params=pltpu.CompilerParams(
            collective_id=0, has_side_effects=True, vmem_limit_bytes=67043328
        ),
    )(assign, assign.reshape(waves // LANES, LANES), u_spec, v_spec, basis)
    return result.reshape(slots, lev_dev, 2, degrees)


def solution(mesh):
    return jax.shard_map(
        functools.partial(body, mesh.shape["lat"]),
        mesh=mesh,
        in_specs=(
            P(),
            P("lat", "lev", None, None),
            P("lat", "lev", None, None),
            P("lat", "lev", None),
        ),
        out_specs=P("lat", "lev", None, None),
        check_vma=False,
    )
```

```python
import functools
import math

import jax
import jax.numpy as jnp
from jax import lax
from jax.experimental import pallas as pl
from jax.experimental.pallas import tpu as pltpu
from jax.sharding import PartitionSpec as P

LON = 2560
SLOTS = 5
BLOCKS = 5
LANES = 128
GROUP = 16
HALF_LEVELS = 8
ORDER = (2, 1, 3, 0)
ROWS = 16


def cos_sin(turns):
    x = turns - jnp.floor(turns + 0.5)
    u = x * x
    cos = jnp.full_like(u, (2 * math.pi) ** 18 / math.factorial(18) * -1.0)
    sin = jnp.full_like(u, (2 * math.pi) ** 19 / math.factorial(19) * -1.0)
    for i in range(8, -1, -1):
        sign = 1.0 if i % 2 == 0 else -1.0
        cos = cos * u + sign * (2 * math.pi) ** (2 * i) / math.factorial(2 * i)
        sin = sin * u + sign * (2 * math.pi) ** (2 * i + 1) / math.factorial(2 * i + 1)
    return cos, sin * x


def tile_rows(value, count):
    return jnp.concatenate([value] * count, axis=0)


def parity_of(wave):
    return 1.0 - 2.0 * (wave - 2.0 * jnp.floor(0.5 * wave))


def kernel(
    n_lat, half_rows, degrees,
    assign_hbm, lanes_hbm, u_ref, v_ref, basis_ref,
    out_hbm,
    assign_ref, assign_lanes_ref, out_ref,
    wide_basis, u_own, v_own, u_other, v_other, edge_send, edge_recv,
    send, recv, split, cos_coeffs, sin_coeffs, cos_flux, sin_flux, mix, back, ret, sum_send, sum_recv,
    cos_q, sin_q, end_q, cos_k, sin_k, row_waves,
    ready, load_sem, swap_send_sem, swap_recv_sem, edge_send_sem, edge_recv_sem,
    send_sem, recv_sem, local_sem, back_send_sem, back_recv_sem, back_local_sem, sum_send_sem, sum_recv_sem, out_sem,
):
    me = lax.axis_index("lat")
    lev = lax.axis_index("lev")
    x_hi = lev // 2
    core = lax.rem(lev, 2)
    spread = 2 * lev
    rows_x = 2 * half_rows
    wide = wide_basis.shape[1]
    waves = SLOTS * n_lat
    half_lon = LON // 2
    units = BLOCKS * GROUP
    mesh_id = pl.DeviceIdType.MESH

    my_group = me // 8
    my_z = lax.rem(lax.rem(me, 8) + 32 - lax.rem(my_group * 3 + spread, 8), 8)
    my_block = (5 * my_z + 7) // 8
    active = (8 * my_block) // 5 == my_z
    my_level = my_group // 2
    my_half = lax.rem(my_group + my_level, 2)

    own_rows = pl.ds(pl.multiple_of(core * half_rows, ROWS), half_rows)
    loads = [
        pltpu.make_async_copy(basis_ref, wide_basis.at[:, own_rows], load_sem.at[0]),
        pltpu.make_async_copy(u_ref, u_own, load_sem.at[1]),
        pltpu.make_async_copy(v_ref, v_own, load_sem.at[2]),
        pltpu.make_async_copy(assign_hbm, assign_ref, load_sem.at[3]),
        pltpu.make_async_copy(lanes_hbm, assign_lanes_ref, load_sem.at[4]),
    ]
    for load in loads:
        load.start()

    barrier = pltpu.get_barrier_semaphore()
    for i in range(1, 4):
        pl.semaphore_signal(barrier, inc=1, device_id={"lev": lax.rem(lev + i, 4)}, device_id_type=mesh_id)
    plane = me - lax.rem(me, GROUP)

    @pl.loop(1, GROUP)
    def _(i):
        peer = plane + lax.rem(me + i, GROUP)
        pl.semaphore_signal(barrier, inc=1, device_id={"lat": peer}, device_id_type=mesh_id)

    planes = n_lat // GROUP

    @pl.loop(1, planes)
    def _(i):
        peer = lax.rem(me + i * GROUP, n_lat)
        pl.semaphore_signal(barrier, inc=1, device_id={"lat": peer}, device_id_type=mesh_id)

    inner = x_hi + core == 1
    loads[0].wait()

    @pl.when(inner & (x_hi == 1))
    def _():
        for k in range(SLOTS):
            edge_send[k] = jnp.broadcast_to(wide_basis[k, 0:ROWS, :][0:1], (2, degrees))

    @pl.when(inner & (x_hi == 0))
    def _():
        for k in range(SLOTS):
            edge_send[k] = jnp.broadcast_to(wide_basis[k, rows_x - ROWS : rows_x, :][ROWS - 1 :], (2, degrees))

    pl.semaphore_wait(barrier, 3 + GROUP - 1 + planes - 1)

    partner = lax.rem(lev + 2, 4)
    sibling = 2 * x_hi + 1 - core

    def swap(i, source, target, device):
        return pltpu.make_async_remote_copy(
            src_ref=source, dst_ref=target, send_sem=swap_send_sem.at[i], recv_sem=swap_recv_sem.at[i],
            device_id={"lev": device}, device_id_type=mesh_id,
        )

    groups = ((0, 3), (3, 2))
    swaps = [
        swap(2 * i + j, own.at[pl.ds(first, count)], other.at[pl.ds(first, count)], partner)
        for i, (first, count) in enumerate(groups)
        for j, (own, other) in enumerate(((u_own, u_other), (v_own, v_other)))
    ]
    swap_basis = swap(4, wide_basis.at[:, own_rows], wide_basis.at[:, own_rows], sibling)

    edge_base = 2 - 2 * x_hi

    def edge_copy(i):
        return pltpu.make_async_remote_copy(
            src_ref=edge_send, dst_ref=edge_recv, send_sem=edge_send_sem.at[i], recv_sem=edge_recv_sem,
            device_id={"lev": edge_base + i}, device_id_type=mesh_id,
        )

    @pl.when(inner)
    def _():
        edge_copy(0).start()
        edge_copy(1).start()

    swap_basis.start()
    @pl.loop(1, planes)
    def _(i):
        peer = lax.rem(me + i * GROUP, n_lat)
        pl.semaphore_signal(ready, inc=1, device_id={"lat": peer}, device_id_type=mesh_id)

    loads[1].wait()
    loads[2].wait()
    for copy in swaps:
        copy.start()
    loads[3].wait()
    loads[4].wait()

    lane_waves = []
    for t in range(waves // LANES):
        line = assign_lanes_ref[t : t + 1, :].astype(jnp.float32)
        lane_waves.append(jnp.broadcast_to(line, (8, LANES)))
        row_waves[t * LANES : (t + 1) * LANES, :] = jnp.broadcast_to(line, (LANES, LANES)).T

    chunk = 64

    @pl.loop(0, waves // chunk)
    def _(i):
        rows = pl.ds(pl.multiple_of(i * chunk, chunk), chunk)
        wave = row_waves[rows, :]
        column = lax.broadcasted_iota(jnp.int32, (chunk, LANES), 1).astype(jnp.float32)
        cos, sin = cos_sin(wave * column * (1.0 / LON))
        turn_cos, turn_sin = cos_sin(wave * (LANES / LON))
        for step in range(half_lon // LANES):
            lanes = slice(step * LANES, (step + 1) * LANES)
            cos_k[rows, lanes] = cos.astype(jnp.bfloat16)
            sin_k[rows, lanes] = sin.astype(jnp.bfloat16)
            cos, sin = cos * turn_cos - sin * turn_sin, sin * turn_cos + cos * turn_sin

    edge_copy(0).wait_recv()
    for k in range(SLOTS):
        wide_basis[k, rows_x:wide, :] = jnp.broadcast_to(edge_recv[k][0:1], (wide - rows_x, degrees))
    swap_basis.wait()

    send_rows = send.reshape(2, BLOCKS, SLOTS, 2, ROWS, LANES)
    lane = lax.broadcasted_iota(jnp.int32, (2 * ROWS, wide), 1)
    row = lax.broadcasted_iota(jnp.int32, (2 * ROWS, wide), 0)
    half_sign = jnp.where(row < ROWS, -0.5, 0.5)
    even = lax.rem(row, 2) == 0
    lane_tile = lax.broadcasted_iota(jnp.int32, (ROWS, LANES), 1)
    degree = lax.broadcasted_iota(jnp.int32, (8, degrees), 1)
    degree_sign = (1 - 2 * lax.rem(degree, 2)).astype(jnp.float32)

    def factors(k):
        wave = assign_ref[me * SLOTS + k]
        parity = (1 - 2 * lax.rem(wave, 2)).astype(jnp.float32)
        live = jnp.where(degree >= wave, 1.0, 0.0)
        return wave, parity, live, live * (parity * degree_sign)

    def meridional(half, u_rows, v_rows, first, count):
        for k in range(first, first + count):
            wave, parity, live, signed = factors(k)
            live = tile_rows(live, 2).astype(jnp.bfloat16)
            signed = tile_rows(signed, 2).astype(jnp.bfloat16)
            u, v = u_rows[k], v_rows[k]
            lhs = jnp.concatenate([u * live, u * signed, v * live, v * signed], axis=0)
            fields = lax.dot_general(
                wide_basis[k], lhs, (((1,), (1,)), ((), ())), preferred_element_type=jnp.float32
            ).T
            wind, other = fields[: 2 * ROWS], fields[2 * ROWS :]
            turned = jnp.where(even, pltpu.roll(other, 2 * ROWS - 1, 0), -pltpu.roll(other, 1, 0))
            sine = cos_sin(jnp.full((8, wide), 1.0 / LON, jnp.float32) * wave.astype(jnp.float32))[1]
            before = pltpu.roll(wind, 1, 1)
            after = pltpu.roll(wind, wide - 1, 1)
            swapped = jnp.concatenate([wind[ROWS:], wind[:ROWS]], axis=0)
            before = jnp.where((lane == 0) & (x_hi == 0), -parity * wind, before)
            after = jnp.where((lane == rows_x - 1) & (x_hi == 1), swapped, after)
            curl = tile_rows(sine, 2 * ROWS // 8) * turned + half_sign * (before - after)
            for f, value in enumerate((wind, curl)):
                north, south = value[:ROWS], value[ROWS:]
                tail = 2 * LANES
                mixed = jnp.where(
                    lane_tile < LANES // 2,
                    north[:, tail : tail + LANES],
                    pltpu.roll(south[:, tail : tail + LANES], LANES // 2, 1),
                )
                tiles = (north[:, :LANES], north[:, LANES:tail], south[:, :LANES], south[:, LANES:tail], mixed)
                for b, tile in enumerate(tiles):
                    send_rows[f, b, k, half] = tile.astype(jnp.bfloat16)

    def send_half(half):
        def send_unit(block, group, level, turn):
            owner = group * 8 + lax.rem((8 * block) // 5 + turn, 8)
            return owner, pltpu.make_async_remote_copy(
                src_ref=send.at[:, block, :, half, level], dst_ref=recv.at[:, me], send_sem=send_sem, recv_sem=recv_sem,
                device_id={"lat": owner}, device_id_type=mesh_id,
            )

        def place(level):
            group = level * 2 + lax.rem(level + half, 2)
            return group, lax.rem(group * 3 + spread, 8)

        for i in (4, 3, 5, 2, 6, 1, 7):
            level = lax.rem(my_level + i, HALF_LEVELS)
            group, turn = place(level)
            for block in range(BLOCKS):
                send_unit(block, group, level, turn)[1].start()

        group, turn = place(my_level)
        for block in range(BLOCKS):
            owner, copy = send_unit(block, group, my_level, turn)

            @pl.when(owner != me)
            def _():
                copy.start()

            @pl.when(owner == me)
            def _():
                pltpu.make_async_copy(send.at[:, block, :, half, my_level], recv.at[:, me], local_sem).start()

    meridional(0, u_own.reshape(SLOTS, ROWS, degrees), v_own.reshape(SLOTS, ROWS, degrees), 0, SLOTS)
    pl.semaphore_wait(ready, planes - 1)
    send_half(0)

    for i, (first, count) in enumerate(groups):
        swaps[2 * i].wait()
        swaps[2 * i + 1].wait()
        meridional(
            1, u_other.reshape(SLOTS, ROWS, degrees), v_other.reshape(SLOTS, ROWS, degrees), first, count
        )
    send_half(1)

    wave = jnp.concatenate(lane_waves, axis=1)
    end_q[...] = tile_rows(parity_of(wave), ROWS // 8).astype(jnp.bfloat16)
    turn_cos, turn_sin = cos_sin(wave * (ROWS / LON))
    turn_cos, turn_sin = tile_rows(turn_cos, ROWS // 8), tile_rows(turn_sin, ROWS // 8)
    position = lax.broadcasted_iota(jnp.int32, (ROWS, waves), 0).astype(jnp.float32)

    def advance(i, carry):
        cos, sin = carry
        rows = pl.ds(pl.multiple_of(i * ROWS, ROWS), ROWS)
        cos_q[rows, :] = cos.astype(jnp.bfloat16)
        sin_q[rows, :] = sin.astype(jnp.bfloat16)
        return cos * turn_cos - sin * turn_sin, sin * turn_cos + cos * turn_sin

    lax.fori_loop(0, half_lon // ROWS, advance, cos_sin(tile_rows(wave, ROWS // 8) * position * (1.0 / LON)))

    @pl.when(inner)
    def _():
        edge_copy(0).wait_send()
        edge_copy(1).wait_send()

    @pl.when(active)
    def _():
        remote = recv.at[:, pl.ds(0, n_lat - 1)]
        pltpu.make_async_copy(remote, remote, recv_sem).wait()
        pltpu.make_async_copy(recv.at[:, 0], recv.at[:, 0], local_sem).wait()
        recv_rows = recv.reshape(2, 2 * waves, LANES)
        for f in range(2):
            lanes = slice(f * LANES, (f + 1) * LANES)
            split[f] = recv_rows[f].astype(jnp.float32)
            cos_coeffs[:, lanes] = split[f, pl.ds(0, waves, 2), :].astype(jnp.bfloat16)
            sin_coeffs[:, lanes] = split[f, pl.ds(1, waves, 2), :].astype(jnp.bfloat16)
        step = 640
        first_row = lax.broadcasted_iota(jnp.int32, (step, LANES), 0)

        @pl.loop(0, half_lon // step)
        def _(i):
            rows = pl.ds(pl.multiple_of(i * step, step), step)
            cos = jnp.dot(cos_q[rows, :], cos_coeffs[...], preferred_element_type=jnp.float32)
            sin = jnp.dot(sin_q[rows, :], sin_coeffs[...], preferred_element_type=jnp.float32)
            cos_u, cos_w = cos[:, :LANES], cos[:, LANES:]
            sin_u, sin_w = sin[:, :LANES], sin[:, LANES:]
            share = jnp.where(first_row + i * step == 0, 0.5, 1.0)
            cos_flux[rows, :] = (share * (cos_u * cos_w + sin_u * sin_w)).astype(jnp.bfloat16)
            sin_flux[rows, :] = (cos_u * sin_w + sin_u * cos_w).astype(jnp.bfloat16)

        end = jnp.dot(end_q[...], cos_coeffs[...], preferred_element_type=jnp.float32)
        end_flux = 0.5 * end[0:1, :LANES] * end[0:1, LANES:]

        back_rows = back.reshape(2 * waves, LANES)
        pieces = len(ORDER)
        owners = n_lat // pieces
        high = waves // pieces
        scale = 2.0 / math.sqrt(LON)

        target = ret.at[my_block, :, my_half, my_level]
        my_piece = me // owners
        my_place = lax.rem(me, owners)
        for i, offset in enumerate(ORDER):
            piece = lax.rem(my_piece + offset, pieces)
            rows = pl.ds(pl.multiple_of(piece * high, high), high)
            cos = jnp.dot(cos_k[rows, :], cos_flux[...], preferred_element_type=jnp.float32)
            sin = jnp.dot(sin_k[rows, :], sin_flux[...], preferred_element_type=jnp.float32)
            cos = cos + parity_of(row_waves[rows, :]) * end_flux
            mix[i, pl.ds(0, high, 2), :] = cos * scale
            mix[i, pl.ds(1, high, 2), :] = sin * scale
            both = pl.ds(pl.multiple_of(piece * 2 * high, 2 * high), 2 * high)
            back_rows[both, :] = mix[i].astype(jnp.bfloat16)
            if i == pieces - 1:
                pltpu.make_async_copy(back.at[me], target, back_local_sem).start()
            for j in range(1 if i == pieces - 1 else 0, owners):
                owner = piece * owners + lax.rem(my_place + j, owners)
                pltpu.make_async_remote_copy(
                    src_ref=back.at[owner], dst_ref=target, send_sem=back_send_sem, recv_sem=back_recv_sem,
                    device_id={"lat": owner}, device_id_type=mesh_id,
                ).start()

        pltpu.make_async_copy(back.at[me], back.at[me], back_local_sem).wait()
        sent = recv.at[:, pl.ds(0, units - 1)]
        pltpu.make_async_copy(sent, sent, send_sem).wait()
        got = recv.at[0, pl.ds(0, units - 1)]
        pltpu.make_async_copy(got, got, back_recv_sem).wait()

    @pl.when(jnp.logical_not(active))
    def _():
        sent = recv.at[:, pl.ds(0, units)]
        pltpu.make_async_copy(sent, sent, send_sem).wait()
        got = recv.at[0, pl.ds(0, units)]
        pltpu.make_async_copy(got, got, back_recv_sem).wait()

    out_rows = out_ref.reshape(SLOTS, ROWS, degrees)
    ret_rows = ret.reshape(BLOCKS, SLOTS, 2 * ROWS, LANES)
    wide_lane = lax.broadcasted_iota(jnp.int32, (2 * ROWS, LANES), 1)

    def sum_copy(k):
        return pltpu.make_async_remote_copy(
            src_ref=sum_send.at[k], dst_ref=sum_recv.at[k],
            send_sem=sum_send_sem.at[k], recv_sem=sum_recv_sem.at[k],
            device_id={"lev": partner}, device_id_type=mesh_id,
        )

    for k in range(SLOTS):
        wave, parity, live, signed = factors(k)
        mixed = ret_rows[4, k].astype(jnp.float32)
        zero = jnp.zeros_like(mixed)
        tail_north = jnp.where(wide_lane < LANES // 2, mixed, zero).astype(jnp.bfloat16)
        tail_south = jnp.where(wide_lane < LANES // 2, pltpu.roll(mixed, LANES // 2, 1), zero).astype(jnp.bfloat16)
        north = jnp.concatenate([ret_rows[0, k], ret_rows[1, k], tail_north], axis=1)
        south = jnp.concatenate([ret_rows[2, k], ret_rows[3, k], tail_south], axis=1)
        both = jnp.dot(
            jnp.concatenate([north, south], axis=0), wide_basis[k], preferred_element_type=jnp.float32
        )
        combined = tile_rows(live, 4) * both[: 2 * ROWS] + tile_rows(signed, 4) * both[2 * ROWS :]
        sum_send[k] = combined[ROWS:].astype(jnp.bfloat16)
        sum_copy(k).start()
        out_rows[k] = combined[:ROWS]

    @pl.when(active)
    def _():
        sent = recv.at[0, pl.ds(0, n_lat - 1)]
        pltpu.make_async_copy(sent, sent, back_send_sem).wait()

    stores = [pltpu.make_async_copy(out_ref.at[k], out_hbm.at[k], out_sem.at[k]) for k in range(SLOTS)]
    for k in range(SLOTS):
        sum_copy(k).wait()
        out_rows[k] += sum_recv[k].astype(jnp.float32)
        stores[k].start()
    for store in stores:
        store.wait()


def body(n_lat, assign, u_spec, v_spec, basis):
    slots, lev_dev, _, degrees = u_spec.shape
    half_rows = basis.shape[1]
    waves = assign.shape[0]
    wide = 3 * LANES

    hbm = pl.BlockSpec(memory_space=pltpu.HBM)
    bf16 = jnp.bfloat16
    f32 = jnp.float32
    dma = pltpu.SemaphoreType.DMA
    result = pl.pallas_call(
        functools.partial(kernel, n_lat, half_rows, degrees),
        out_shape=jax.ShapeDtypeStruct((slots, lev_dev, 2, degrees), jnp.float32),
        in_specs=[hbm] * 5,
        out_specs=hbm,
        scratch_shapes=[
            pltpu.SMEM((waves,), jnp.int32),
            pltpu.VMEM((waves // LANES, LANES), jnp.int32),
            pltpu.VMEM((slots, lev_dev, 2, degrees), f32),
            pltpu.VMEM((slots, wide, degrees), bf16),
            pltpu.VMEM((slots, lev_dev, 2, degrees), bf16),
            pltpu.VMEM((slots, lev_dev, 2, degrees), bf16),
            pltpu.VMEM((slots, lev_dev, 2, degrees), bf16),
            pltpu.VMEM((slots, lev_dev, 2, degrees), bf16),
            pltpu.VMEM((slots, 2, degrees), bf16),
            pltpu.VMEM((slots, 2, degrees), bf16),
            pltpu.VMEM((2, BLOCKS, SLOTS, 2, HALF_LEVELS, 2, LANES), bf16),
            pltpu.VMEM((2, n_lat, SLOTS, 2, LANES), bf16),
            pltpu.VMEM((2, 2 * waves, LANES), f32),
            pltpu.VMEM((waves, 2 * LANES), bf16),
            pltpu.VMEM((waves, 2 * LANES), bf16),
            pltpu.VMEM((LON // 2, LANES), bf16),
            pltpu.VMEM((LON // 2, LANES), bf16),
            pltpu.VMEM((len(ORDER), 2 * waves // len(ORDER), LANES), f32),
            pltpu.VMEM((n_lat, SLOTS, 2, LANES), bf16),
            pltpu.VMEM((BLOCKS, SLOTS, 2, HALF_LEVELS, 2, LANES), bf16),
            pltpu.VMEM((SLOTS, ROWS, degrees), bf16),
            pltpu.VMEM((SLOTS, ROWS, degrees), bf16),
            pltpu.VMEM((LON // 2, waves), bf16),
            pltpu.VMEM((LON // 2, waves), bf16),
            pltpu.VMEM((ROWS, waves), bf16),
            pltpu.VMEM((waves, LON // 2), bf16),
            pltpu.VMEM((waves, LON // 2), bf16),
            pltpu.VMEM((waves, LANES), f32),
            pltpu.SemaphoreType.REGULAR,
            dma((5,)), dma((5,)), dma((5,)), dma((2,)), dma,
            dma, dma, dma, dma, dma, dma, dma((SLOTS,)), dma((SLOTS,)), dma((SLOTS,)),
        ],
        compiler_params=pltpu.CompilerParams(
            collective_id=0, has_side_effects=True, vmem_limit_bytes=67043328
        ),
    )(assign, assign.reshape(waves // LANES, LANES), u_spec, v_spec, basis)
    return result


def solution(mesh):
    return jax.shard_map(
        functools.partial(body, mesh.shape["lat"]),
        mesh=mesh,
        in_specs=(
            P(),
            P("lat", "lev", None, None),
            P("lat", "lev", None, None),
            P("lat", "lev", None),
        ),
        out_specs=P("lat", "lev", None, None),
        check_vma=False,
    )
```

```python
import functools
import math

import jax
import jax.numpy as jnp
from jax import lax
from jax.experimental import pallas as pl
from jax.experimental.pallas import tpu as pltpu
from jax.sharding import PartitionSpec as P

LON = 2560
SLOTS = 5
BLOCKS = 5
LANES = 128
GROUP = 16
HALF_LEVELS = 8
ORDER = (2, 1, 3, 0)
ROWS = 16


def cos_sin(turns):
    x = turns - jnp.floor(turns + 0.5)
    u = x * x
    cos = jnp.full_like(u, (2 * math.pi) ** 18 / math.factorial(18) * -1.0)
    sin = jnp.full_like(u, (2 * math.pi) ** 19 / math.factorial(19) * -1.0)
    for i in range(8, -1, -1):
        sign = 1.0 if i % 2 == 0 else -1.0
        cos = cos * u + sign * (2 * math.pi) ** (2 * i) / math.factorial(2 * i)
        sin = sin * u + sign * (2 * math.pi) ** (2 * i + 1) / math.factorial(2 * i + 1)
    return cos, sin * x


def tile_rows(value, count):
    return jnp.concatenate([value] * count, axis=0)


def parity_of(wave):
    return 1.0 - 2.0 * (wave - 2.0 * jnp.floor(0.5 * wave))


def kernel(
    n_lat, half_rows, degrees,
    assign_hbm, lanes_hbm, u_ref, v_ref, basis_ref,
    out_hbm, sum_hbm,
    assign_ref, assign_lanes_ref, out_ref,
    wide_basis, u_own, v_own, u_other, v_other, edge_send, edge_recv,
    send, recv, split, cos_coeffs, sin_coeffs, cos_flux, sin_flux, mix, back, ret, sum_send,
    cos_q, sin_q, end_q, cos_k, sin_k, row_waves,
    ready, load_sem, swap_send_sem, swap_recv_sem, edge_send_sem, edge_recv_sem,
    send_sem, recv_sem, local_sem, back_send_sem, back_recv_sem, back_local_sem, sum_send_sem, sum_recv_sem, out_sem,
):
    me = lax.axis_index("lat")
    lev = lax.axis_index("lev")
    x_hi = lev // 2
    core = lax.rem(lev, 2)
    rows_x = 2 * half_rows
    wide = wide_basis.shape[1]
    waves = SLOTS * n_lat
    half_lon = LON // 2
    units = BLOCKS * GROUP
    mesh_id = pl.DeviceIdType.MESH

    def turn_of(level):
        return lax.rem(5 * level + 4 * core, 8)

    my_level = me // GROUP
    my_z = lax.rem(lax.rem(me, 8) + 8 - turn_of(my_level), 8)
    my_block = (5 * my_z + 7) // 8
    active = (8 * my_block) // 5 == my_z
    my_half = lax.rem(lax.rem(me // 8, 2) + my_block + my_level, 2)

    own_rows = pl.ds(pl.multiple_of(core * half_rows, ROWS), half_rows)
    loads = [
        pltpu.make_async_copy(basis_ref, wide_basis.at[:, own_rows], load_sem.at[0]),
        pltpu.make_async_copy(u_ref, u_own, load_sem.at[1]),
        pltpu.make_async_copy(v_ref, v_own, load_sem.at[2]),
        pltpu.make_async_copy(assign_hbm, assign_ref, load_sem.at[3]),
        pltpu.make_async_copy(lanes_hbm, assign_lanes_ref, load_sem.at[4]),
    ]
    for load in loads:
        load.start()

    barrier = pltpu.get_barrier_semaphore()
    for i in range(1, 4):
        pl.semaphore_signal(barrier, inc=1, device_id={"lev": lax.rem(lev + i, 4)}, device_id_type=mesh_id)
    plane = me - lax.rem(me, GROUP)

    @pl.loop(1, GROUP)
    def _(i):
        peer = plane + lax.rem(me + i, GROUP)
        pl.semaphore_signal(barrier, inc=1, device_id={"lat": peer}, device_id_type=mesh_id)

    planes = n_lat // GROUP

    @pl.loop(1, planes)
    def _(i):
        peer = lax.rem(me + i * GROUP, n_lat)
        pl.semaphore_signal(barrier, inc=1, device_id={"lat": peer}, device_id_type=mesh_id)

    inner = x_hi + core == 1
    loads[0].wait()

    @pl.when(inner & (x_hi == 1))
    def _():
        for k in range(SLOTS):
            edge_send[k] = jnp.broadcast_to(wide_basis[k, 0:ROWS, :][0:1], (2, degrees))

    @pl.when(inner & (x_hi == 0))
    def _():
        for k in range(SLOTS):
            edge_send[k] = jnp.broadcast_to(wide_basis[k, rows_x - ROWS : rows_x, :][ROWS - 1 :], (2, degrees))

    pl.semaphore_wait(barrier, 3 + GROUP - 1 + planes - 1)

    partner = lax.rem(lev + 2, 4)
    sibling = 2 * x_hi + 1 - core

    def swap(i, source, target, device):
        return pltpu.make_async_remote_copy(
            src_ref=source, dst_ref=target, send_sem=swap_send_sem.at[i], recv_sem=swap_recv_sem.at[i],
            device_id={"lev": device}, device_id_type=mesh_id,
        )

    groups = ((0, 3), (3, 2))
    swaps = [
        swap(2 * i + j, own.at[pl.ds(first, count)], other.at[pl.ds(first, count)], partner)
        for i, (first, count) in enumerate(groups)
        for j, (own, other) in enumerate(((u_own, u_other), (v_own, v_other)))
    ]
    swap_basis = swap(4, wide_basis.at[:, own_rows], wide_basis.at[:, own_rows], sibling)

    edge_base = 2 - 2 * x_hi

    def edge_copy(i):
        return pltpu.make_async_remote_copy(
            src_ref=edge_send, dst_ref=edge_recv, send_sem=edge_send_sem.at[i], recv_sem=edge_recv_sem,
            device_id={"lev": edge_base + i}, device_id_type=mesh_id,
        )

    @pl.when(inner)
    def _():
        edge_copy(0).start()
        edge_copy(1).start()

    swap_basis.start()
    @pl.loop(1, planes)
    def _(i):
        peer = lax.rem(me + i * GROUP, n_lat)
        pl.semaphore_signal(ready, inc=1, device_id={"lat": peer}, device_id_type=mesh_id)

    loads[1].wait()
    loads[2].wait()
    for copy in swaps:
        copy.start()
    loads[3].wait()
    loads[4].wait()

    lane_waves = []
    for t in range(waves // LANES):
        line = assign_lanes_ref[t : t + 1, :].astype(jnp.float32)
        lane_waves.append(jnp.broadcast_to(line, (8, LANES)))
        row_waves[t * LANES : (t + 1) * LANES, :] = jnp.broadcast_to(line, (LANES, LANES)).T

    chunk = 64

    @pl.loop(0, waves // chunk)
    def _(i):
        rows = pl.ds(pl.multiple_of(i * chunk, chunk), chunk)
        wave = row_waves[rows, :]
        column = lax.broadcasted_iota(jnp.int32, (chunk, LANES), 1).astype(jnp.float32)
        cos, sin = cos_sin(wave * column * (1.0 / LON))
        turn_cos, turn_sin = cos_sin(wave * (LANES / LON))
        for step in range(half_lon // LANES):
            lanes = slice(step * LANES, (step + 1) * LANES)
            cos_k[rows, lanes] = cos.astype(jnp.bfloat16)
            sin_k[rows, lanes] = sin.astype(jnp.bfloat16)
            cos, sin = cos * turn_cos - sin * turn_sin, sin * turn_cos + cos * turn_sin

    edge_copy(0).wait_recv()
    for k in range(SLOTS):
        wide_basis[k, rows_x:wide, :] = jnp.broadcast_to(edge_recv[k][0:1], (wide - rows_x, degrees))
    swap_basis.wait()

    send_rows = send.reshape(2, BLOCKS, SLOTS, 2, ROWS, LANES)
    lane = lax.broadcasted_iota(jnp.int32, (2 * ROWS, wide), 1)
    row = lax.broadcasted_iota(jnp.int32, (2 * ROWS, wide), 0)
    half_sign = jnp.where(row < ROWS, -0.5, 0.5)
    even = lax.rem(row, 2) == 0
    lane_tile = lax.broadcasted_iota(jnp.int32, (ROWS, LANES), 1)
    degree = lax.broadcasted_iota(jnp.int32, (8, degrees), 1)
    degree_sign = (1 - 2 * lax.rem(degree, 2)).astype(jnp.float32)

    def factors(k):
        wave = assign_ref[me * SLOTS + k]
        parity = (1 - 2 * lax.rem(wave, 2)).astype(jnp.float32)
        live = jnp.where(degree >= wave, 1.0, 0.0)
        return wave, parity, live, live * (parity * degree_sign)

    def meridional(half, u_rows, v_rows, first, count):
        for k in range(first, first + count):
            wave, parity, live, signed = factors(k)
            live = tile_rows(live, 2).astype(jnp.bfloat16)
            signed = tile_rows(signed, 2).astype(jnp.bfloat16)
            u, v = u_rows[k], v_rows[k]
            lhs = jnp.concatenate([u * live, u * signed, v * live, v * signed], axis=0)
            fields = lax.dot_general(
                wide_basis[k], lhs, (((1,), (1,)), ((), ())), preferred_element_type=jnp.float32
            ).T
            wind, other = fields[: 2 * ROWS], fields[2 * ROWS :]
            turned = jnp.where(even, pltpu.roll(other, 2 * ROWS - 1, 0), -pltpu.roll(other, 1, 0))
            sine = cos_sin(jnp.full((8, wide), 1.0 / LON, jnp.float32) * wave.astype(jnp.float32))[1]
            before = pltpu.roll(wind, 1, 1)
            after = pltpu.roll(wind, wide - 1, 1)
            swapped = jnp.concatenate([wind[ROWS:], wind[:ROWS]], axis=0)
            before = jnp.where((lane == 0) & (x_hi == 0), -parity * wind, before)
            after = jnp.where((lane == rows_x - 1) & (x_hi == 1), swapped, after)
            curl = tile_rows(sine, 2 * ROWS // 8) * turned + half_sign * (before - after)
            for f, value in enumerate((wind, curl)):
                north, south = value[:ROWS], value[ROWS:]
                tail = 2 * LANES
                mixed = jnp.where(
                    lane_tile < LANES // 2,
                    north[:, tail : tail + LANES],
                    pltpu.roll(south[:, tail : tail + LANES], LANES // 2, 1),
                )
                tiles = (north[:, :LANES], north[:, LANES:tail], south[:, :LANES], south[:, LANES:tail], mixed)
                for b, tile in enumerate(tiles):
                    send_rows[f, b, k, half] = tile.astype(jnp.bfloat16)

    def send_half(half):
        def send_unit(block, level, sides, turn):
            owner = sides[block % 2] + lax.rem((8 * block) // 5 + turn, 8)
            return owner, pltpu.make_async_remote_copy(
                src_ref=send.at[:, block, :, half, level], dst_ref=recv.at[:, me], send_sem=send_sem, recv_sem=recv_sem,
                device_id={"lat": owner}, device_id_type=mesh_id,
            )

        def place(level):
            sides = [level * GROUP + 8 * lax.rem(level + half + p, 2) for p in range(2)]
            return sides, turn_of(level)

        for i in (4, 3, 5, 2, 6, 1, 7):
            level = lax.rem(my_level + i, HALF_LEVELS)
            sides, turn = place(level)
            for block in range(BLOCKS):
                send_unit(block, level, sides, turn)[1].start()

        sides, turn = place(my_level)
        for block in range(BLOCKS):
            owner, copy = send_unit(block, my_level, sides, turn)

            @pl.when(owner != me)
            def _():
                copy.start()

            @pl.when(owner == me)
            def _():
                pltpu.make_async_copy(send.at[:, block, :, half, my_level], recv.at[:, me], local_sem).start()

    meridional(0, u_own.reshape(SLOTS, ROWS, degrees), v_own.reshape(SLOTS, ROWS, degrees), 0, SLOTS)
    pl.semaphore_wait(ready, planes - 1)
    send_half(0)

    for i, (first, count) in enumerate(groups):
        swaps[2 * i].wait()
        swaps[2 * i + 1].wait()
        meridional(
            1, u_other.reshape(SLOTS, ROWS, degrees), v_other.reshape(SLOTS, ROWS, degrees), first, count
        )
    send_half(1)

    wave = jnp.concatenate(lane_waves, axis=1)
    end_q[...] = tile_rows(parity_of(wave), ROWS // 8).astype(jnp.bfloat16)
    turn_cos, turn_sin = cos_sin(wave * (ROWS / LON))
    turn_cos, turn_sin = tile_rows(turn_cos, ROWS // 8), tile_rows(turn_sin, ROWS // 8)
    position = lax.broadcasted_iota(jnp.int32, (ROWS, waves), 0).astype(jnp.float32)

    def advance(i, carry):
        cos, sin = carry
        rows = pl.ds(pl.multiple_of(i * ROWS, ROWS), ROWS)
        cos_q[rows, :] = cos.astype(jnp.bfloat16)
        sin_q[rows, :] = sin.astype(jnp.bfloat16)
        return cos * turn_cos - sin * turn_sin, sin * turn_cos + cos * turn_sin

    lax.fori_loop(0, half_lon // ROWS, advance, cos_sin(tile_rows(wave, ROWS // 8) * position * (1.0 / LON)))

    @pl.when(inner)
    def _():
        edge_copy(0).wait_send()
        edge_copy(1).wait_send()

    @pl.when(active)
    def _():
        remote = recv.at[:, pl.ds(0, n_lat - 1)]
        pltpu.make_async_copy(remote, remote, recv_sem).wait()
        pltpu.make_async_copy(recv.at[:, 0], recv.at[:, 0], local_sem).wait()
        recv_rows = recv.reshape(2, 2 * waves, LANES)
        for f in range(2):
            lanes = slice(f * LANES, (f + 1) * LANES)
            split[f] = recv_rows[f].astype(jnp.float32)
            cos_coeffs[:, lanes] = split[f, pl.ds(0, waves, 2), :].astype(jnp.bfloat16)
            sin_coeffs[:, lanes] = split[f, pl.ds(1, waves, 2), :].astype(jnp.bfloat16)
        step = 640
        first_row = lax.broadcasted_iota(jnp.int32, (step, LANES), 0)

        @pl.loop(0, half_lon // step)
        def _(i):
            rows = pl.ds(pl.multiple_of(i * step, step), step)
            cos = jnp.dot(cos_q[rows, :], cos_coeffs[...], preferred_element_type=jnp.float32)
            sin = jnp.dot(sin_q[rows, :], sin_coeffs[...], preferred_element_type=jnp.float32)
            cos_u, cos_w = cos[:, :LANES], cos[:, LANES:]
            sin_u, sin_w = sin[:, :LANES], sin[:, LANES:]
            share = jnp.where(first_row + i * step == 0, 0.5, 1.0)
            cos_flux[rows, :] = (share * (cos_u * cos_w + sin_u * sin_w)).astype(jnp.bfloat16)
            sin_flux[rows, :] = (cos_u * sin_w + sin_u * cos_w).astype(jnp.bfloat16)

        end = jnp.dot(end_q[...], cos_coeffs[...], preferred_element_type=jnp.float32)
        end_flux = 0.5 * end[0:1, :LANES] * end[0:1, LANES:]

        back_rows = back.reshape(2 * waves, LANES)
        pieces = len(ORDER)
        owners = n_lat // pieces
        high = waves // pieces
        scale = 2.0 / math.sqrt(LON)

        target = ret.at[my_block, :, my_half, my_level]
        my_piece = me // owners
        my_place = lax.rem(me, owners)
        for i, offset in enumerate(ORDER):
            piece = lax.rem(my_piece + offset, pieces)
            rows = pl.ds(pl.multiple_of(piece * high, high), high)
            cos = jnp.dot(cos_k[rows, :], cos_flux[...], preferred_element_type=jnp.float32)
            sin = jnp.dot(sin_k[rows, :], sin_flux[...], preferred_element_type=jnp.float32)
            cos = cos + parity_of(row_waves[rows, :]) * end_flux
            mix[i, pl.ds(0, high, 2), :] = cos * scale
            mix[i, pl.ds(1, high, 2), :] = sin * scale
            both = pl.ds(pl.multiple_of(piece * 2 * high, 2 * high), 2 * high)
            back_rows[both, :] = mix[i].astype(jnp.bfloat16)
            if i == pieces - 1:
                pltpu.make_async_copy(back.at[me], target, back_local_sem).start()
            for j in range(1 if i == pieces - 1 else 0, owners):
                owner = piece * owners + lax.rem(my_place + j, owners)
                pltpu.make_async_remote_copy(
                    src_ref=back.at[owner], dst_ref=target, send_sem=back_send_sem, recv_sem=back_recv_sem,
                    device_id={"lat": owner}, device_id_type=mesh_id,
                ).start()

        pltpu.make_async_copy(back.at[me], back.at[me], back_local_sem).wait()
        sent = recv.at[:, pl.ds(0, units - 1)]
        pltpu.make_async_copy(sent, sent, send_sem).wait()
        got = recv.at[0, pl.ds(0, units - 1)]
        pltpu.make_async_copy(got, got, back_recv_sem).wait()

    @pl.when(jnp.logical_not(active))
    def _():
        sent = recv.at[:, pl.ds(0, units)]
        pltpu.make_async_copy(sent, sent, send_sem).wait()
        got = recv.at[0, pl.ds(0, units)]
        pltpu.make_async_copy(got, got, back_recv_sem).wait()

    out_rows = out_ref.reshape(SLOTS, ROWS, degrees)
    sum_rows = sum_send.reshape(SLOTS, ROWS, degrees)
    stores = [pltpu.make_async_copy(out_ref.at[k], out_hbm.at[k], out_sem.at[k]) for k in range(SLOTS)]
    ret_rows = ret.reshape(BLOCKS, SLOTS, 2 * ROWS, LANES)
    wide_lane = lax.broadcasted_iota(jnp.int32, (2 * ROWS, LANES), 1)

    def sum_copy(k):
        return pltpu.make_async_remote_copy(
            src_ref=sum_send.at[k], dst_ref=sum_hbm.at[k],
            send_sem=sum_send_sem.at[k], recv_sem=sum_recv_sem.at[k],
            device_id={"lev": partner}, device_id_type=mesh_id,
        )

    for k in range(SLOTS):
        wave, parity, live, signed = factors(k)
        mixed = ret_rows[4, k].astype(jnp.float32)
        zero = jnp.zeros_like(mixed)
        tail_north = jnp.where(wide_lane < LANES // 2, mixed, zero).astype(jnp.bfloat16)
        tail_south = jnp.where(wide_lane < LANES // 2, pltpu.roll(mixed, LANES // 2, 1), zero).astype(jnp.bfloat16)
        north = jnp.concatenate([ret_rows[0, k], ret_rows[1, k], tail_north], axis=1)
        south = jnp.concatenate([ret_rows[2, k], ret_rows[3, k], tail_south], axis=1)
        both = jnp.dot(
            jnp.concatenate([north, south], axis=0), wide_basis[k], preferred_element_type=jnp.float32
        )
        combined = tile_rows(live, 4) * both[: 2 * ROWS] + tile_rows(signed, 4) * both[2 * ROWS :]
        sum_rows[k] = combined[ROWS:].astype(jnp.bfloat16)
        sum_copy(k).start()
        out_rows[k] = combined[:ROWS]
        stores[k].start()

    @pl.when(active)
    def _():
        sent = recv.at[0, pl.ds(0, n_lat - 1)]
        pltpu.make_async_copy(sent, sent, back_send_sem).wait()

    for k in range(SLOTS):
        stores[k].wait()
    for k in range(SLOTS):
        sum_copy(k).wait()


def body(n_lat, assign, u_spec, v_spec, basis):
    slots, lev_dev, _, degrees = u_spec.shape
    half_rows = basis.shape[1]
    waves = assign.shape[0]
    wide = 3 * LANES

    hbm = pl.BlockSpec(memory_space=pltpu.HBM)
    bf16 = jnp.bfloat16
    f32 = jnp.float32
    dma = pltpu.SemaphoreType.DMA
    own, other = pl.pallas_call(
        functools.partial(kernel, n_lat, half_rows, degrees),
        out_shape=[jax.ShapeDtypeStruct(u_spec.shape, f32), jax.ShapeDtypeStruct(u_spec.shape, bf16)],
        in_specs=[hbm] * 5,
        out_specs=[hbm, hbm],
        scratch_shapes=[
            pltpu.SMEM((waves,), jnp.int32),
            pltpu.VMEM((waves // LANES, LANES), jnp.int32),
            pltpu.VMEM((slots, lev_dev, 2, degrees), f32),
            pltpu.VMEM((slots, wide, degrees), bf16),
            pltpu.VMEM((slots, lev_dev, 2, degrees), bf16),
            pltpu.VMEM((slots, lev_dev, 2, degrees), bf16),
            pltpu.VMEM((slots, lev_dev, 2, degrees), bf16),
            pltpu.VMEM((slots, lev_dev, 2, degrees), bf16),
            pltpu.VMEM((slots, 2, degrees), bf16),
            pltpu.VMEM((slots, 2, degrees), bf16),
            pltpu.VMEM((2, BLOCKS, SLOTS, 2, HALF_LEVELS, 2, LANES), bf16),
            pltpu.VMEM((2, n_lat, SLOTS, 2, LANES), bf16),
            pltpu.VMEM((2, 2 * waves, LANES), f32),
            pltpu.VMEM((waves, 2 * LANES), bf16),
            pltpu.VMEM((waves, 2 * LANES), bf16),
            pltpu.VMEM((LON // 2, LANES), bf16),
            pltpu.VMEM((LON // 2, LANES), bf16),
            pltpu.VMEM((len(ORDER), 2 * waves // len(ORDER), LANES), f32),
            pltpu.VMEM((n_lat, SLOTS, 2, LANES), bf16),
            pltpu.VMEM((BLOCKS, SLOTS, 2, HALF_LEVELS, 2, LANES), bf16),
            pltpu.VMEM((slots, lev_dev, 2, degrees), bf16),
            pltpu.VMEM((LON // 2, waves), bf16),
            pltpu.VMEM((LON // 2, waves), bf16),
            pltpu.VMEM((ROWS, waves), bf16),
            pltpu.VMEM((waves, LON // 2), bf16),
            pltpu.VMEM((waves, LON // 2), bf16),
            pltpu.VMEM((waves, LANES), f32),
            pltpu.SemaphoreType.REGULAR,
            dma((5,)), dma((5,)), dma((5,)), dma((2,)), dma,
            dma, dma, dma, dma, dma, dma, dma((SLOTS,)), dma((SLOTS,)), dma((SLOTS,)),
        ],
        compiler_params=pltpu.CompilerParams(
            collective_id=0, has_side_effects=True, vmem_limit_bytes=67043328
        ),
    )(assign, assign.reshape(waves // LANES, LANES), u_spec, v_spec, basis)
    return own + other.astype(f32)


def solution(mesh):
    return jax.shard_map(
        functools.partial(body, mesh.shape["lat"]),
        mesh=mesh,
        in_specs=(
            P(),
            P("lat", "lev", None, None),
            P("lat", "lev", None, None),
            P("lat", "lev", None),
        ),
        out_specs=P("lat", "lev", None, None),
        check_vma=False,
    )
```

```python
import functools
import math

import jax
import jax.numpy as jnp
from jax import lax
from jax.experimental import pallas as pl
from jax.experimental.pallas import tpu as pltpu
from jax.sharding import PartitionSpec as P

LON = 2560
SLOTS = 5
BLOCKS = 5
LANES = 128
GROUP = 16
HALF_LEVELS = 8
ORDER = (2, 1, 3, 0)
ROWS = 16


def cos_sin(turns):
    x = turns - jnp.floor(turns + 0.5)
    u = x * x
    cos = jnp.full_like(u, (2 * math.pi) ** 18 / math.factorial(18) * -1.0)
    sin = jnp.full_like(u, (2 * math.pi) ** 19 / math.factorial(19) * -1.0)
    for i in range(8, -1, -1):
        sign = 1.0 if i % 2 == 0 else -1.0
        cos = cos * u + sign * (2 * math.pi) ** (2 * i) / math.factorial(2 * i)
        sin = sin * u + sign * (2 * math.pi) ** (2 * i + 1) / math.factorial(2 * i + 1)
    return cos, sin * x


def tile_rows(value, count):
    return jnp.concatenate([value] * count, axis=0)


def parity_of(wave):
    return 1.0 - 2.0 * (wave - 2.0 * jnp.floor(0.5 * wave))


def kernel(
    n_lat, half_rows, degrees,
    assign_hbm, lanes_hbm, u_ref, v_ref, basis_ref,
    out_hbm, sum_hbm,
    assign_ref, assign_lanes_ref, out_ref,
    wide_basis, u_own, v_own, u_other, v_other, edge_send, edge_recv,
    send, recv, split, cos_coeffs, sin_coeffs, cos_flux, sin_flux, mix, back, ret, sum_send,
    cos_q, sin_q, end_q, cos_k, sin_k, row_waves,
    ready, load_sem, swap_send_sem, swap_recv_sem, edge_send_sem, edge_recv_sem,
    send_sem, recv_sem, local_sem, back_send_sem, back_recv_sem, back_local_sem, sum_send_sem, sum_recv_sem, out_sem,
):
    me = lax.axis_index("lat")
    lev = lax.axis_index("lev")
    x_hi = lev // 2
    core = lax.rem(lev, 2)
    rows_x = 2 * half_rows
    wide = wide_basis.shape[1]
    waves = SLOTS * n_lat
    half_lon = LON // 2
    units = BLOCKS * GROUP
    mesh_id = pl.DeviceIdType.MESH

    def turn_of(level):
        return lax.rem(5 * level + 4 * core, 8)

    my_level = me // GROUP
    my_z = lax.rem(lax.rem(me, 8) + 8 - turn_of(my_level), 8)
    my_block = (5 * my_z + 7) // 8
    active = (8 * my_block) // 5 == my_z
    my_half = lax.rem(lax.rem(me // 8, 2) + my_block + my_level, 2)

    own_rows = pl.ds(pl.multiple_of(core * half_rows, ROWS), half_rows)
    loads = [
        pltpu.make_async_copy(basis_ref, wide_basis.at[:, own_rows], load_sem.at[0]),
        pltpu.make_async_copy(u_ref, u_own, load_sem.at[1]),
        pltpu.make_async_copy(v_ref, v_own, load_sem.at[2]),
        pltpu.make_async_copy(assign_hbm, assign_ref, load_sem.at[3]),
        pltpu.make_async_copy(lanes_hbm, assign_lanes_ref, load_sem.at[4]),
    ]
    for load in loads:
        load.start()

    barrier = pltpu.get_barrier_semaphore()
    for i in range(1, 4):
        pl.semaphore_signal(barrier, inc=1, device_id={"lev": lax.rem(lev + i, 4)}, device_id_type=mesh_id)
    plane = me - lax.rem(me, GROUP)

    @pl.loop(1, GROUP)
    def _(i):
        peer = plane + lax.rem(me + i, GROUP)
        pl.semaphore_signal(barrier, inc=1, device_id={"lat": peer}, device_id_type=mesh_id)

    planes = n_lat // GROUP

    @pl.loop(1, planes)
    def _(i):
        peer = lax.rem(me + i * GROUP, n_lat)
        pl.semaphore_signal(barrier, inc=1, device_id={"lat": peer}, device_id_type=mesh_id)

    inner = x_hi + core == 1
    loads[0].wait()

    @pl.when(inner & (x_hi == 1))
    def _():
        for k in range(SLOTS):
            edge_send[k] = jnp.broadcast_to(wide_basis[k, 0:ROWS, :][0:1], (2, degrees))

    @pl.when(inner & (x_hi == 0))
    def _():
        for k in range(SLOTS):
            edge_send[k] = jnp.broadcast_to(wide_basis[k, rows_x - ROWS : rows_x, :][ROWS - 1 :], (2, degrees))

    pl.semaphore_wait(barrier, 3 + GROUP - 1 + planes - 1)

    partner = lax.rem(lev + 2, 4)
    sibling = 2 * x_hi + 1 - core

    def swap(i, source, target, device):
        return pltpu.make_async_remote_copy(
            src_ref=source, dst_ref=target, send_sem=swap_send_sem.at[i], recv_sem=swap_recv_sem.at[i],
            device_id={"lev": device}, device_id_type=mesh_id,
        )

    groups = ((0, 3), (3, 2))
    swaps = [
        swap(2 * i + j, own.at[pl.ds(first, count)], other.at[pl.ds(first, count)], partner)
        for i, (first, count) in enumerate(groups)
        for j, (own, other) in enumerate(((u_own, u_other), (v_own, v_other)))
    ]
    swap_basis = swap(4, wide_basis.at[:, own_rows], wide_basis.at[:, own_rows], sibling)

    edge_base = 2 - 2 * x_hi

    def edge_copy(i):
        return pltpu.make_async_remote_copy(
            src_ref=edge_send, dst_ref=edge_recv, send_sem=edge_send_sem.at[i], recv_sem=edge_recv_sem,
            device_id={"lev": edge_base + i}, device_id_type=mesh_id,
        )

    @pl.when(inner)
    def _():
        edge_copy(0).start()
        edge_copy(1).start()

    swap_basis.start()
    @pl.loop(1, planes)
    def _(i):
        peer = lax.rem(me + i * GROUP, n_lat)
        pl.semaphore_signal(ready, inc=1, device_id={"lat": peer}, device_id_type=mesh_id)

    loads[1].wait()
    loads[2].wait()
    for copy in swaps:
        copy.start()
    loads[3].wait()
    loads[4].wait()

    lane_waves = []
    for t in range(waves // LANES):
        line = assign_lanes_ref[t : t + 1, :].astype(jnp.float32)
        lane_waves.append(jnp.broadcast_to(line, (8, LANES)))
        row_waves[t * LANES : (t + 1) * LANES, :] = jnp.broadcast_to(line, (LANES, LANES)).T

    chunk = 64

    @pl.loop(0, waves // chunk)
    def _(i):
        rows = pl.ds(pl.multiple_of(i * chunk, chunk), chunk)
        wave = row_waves[rows, :]
        column = lax.broadcasted_iota(jnp.int32, (chunk, LANES), 1).astype(jnp.float32)
        cos, sin = cos_sin(wave * column * (1.0 / LON))
        turn_cos, turn_sin = cos_sin(wave * (LANES / LON))
        for step in range(half_lon // LANES):
            lanes = slice(step * LANES, (step + 1) * LANES)
            cos_k[rows, lanes] = cos.astype(jnp.bfloat16)
            sin_k[rows, lanes] = sin.astype(jnp.bfloat16)
            cos, sin = cos * turn_cos - sin * turn_sin, sin * turn_cos + cos * turn_sin

    edge_copy(0).wait_recv()
    for k in range(SLOTS):
        wide_basis[k, rows_x:wide, :] = jnp.broadcast_to(edge_recv[k][0:1], (wide - rows_x, degrees))
    swap_basis.wait()

    send_rows = send.reshape(2, BLOCKS, SLOTS, 2, ROWS, LANES)
    lane = lax.broadcasted_iota(jnp.int32, (2 * ROWS, wide), 1)
    row = lax.broadcasted_iota(jnp.int32, (2 * ROWS, wide), 0)
    half_sign = jnp.where(row < ROWS, -0.5, 0.5)
    even = lax.rem(row, 2) == 0
    lane_tile = lax.broadcasted_iota(jnp.int32, (ROWS, LANES), 1)
    degree = lax.broadcasted_iota(jnp.int32, (8, degrees), 1)
    degree_sign = (1 - 2 * lax.rem(degree, 2)).astype(jnp.float32)

    def factors(k):
        wave = assign_ref[me * SLOTS + k]
        parity = (1 - 2 * lax.rem(wave, 2)).astype(jnp.float32)
        live = jnp.where(degree >= wave, 1.0, 0.0)
        return wave, parity, live, live * (parity * degree_sign)

    def meridional(half, u_rows, v_rows, first, count):
        for k in range(first, first + count):
            wave, parity, live, signed = factors(k)
            live = tile_rows(live, 2).astype(jnp.bfloat16)
            signed = tile_rows(signed, 2).astype(jnp.bfloat16)
            u, v = u_rows[k], v_rows[k]
            lhs = jnp.concatenate([u * live, u * signed, v * live, v * signed], axis=0)
            fields = lax.dot_general(
                wide_basis[k], lhs, (((1,), (1,)), ((), ())), preferred_element_type=jnp.float32
            ).T
            wind, other = fields[: 2 * ROWS], fields[2 * ROWS :]
            turned = jnp.where(even, pltpu.roll(other, 2 * ROWS - 1, 0), -pltpu.roll(other, 1, 0))
            sine = cos_sin(jnp.full((8, wide), 1.0 / LON, jnp.float32) * wave.astype(jnp.float32))[1]
            before = pltpu.roll(wind, 1, 1)
            after = pltpu.roll(wind, wide - 1, 1)
            swapped = jnp.concatenate([wind[ROWS:], wind[:ROWS]], axis=0)
            before = jnp.where((lane == 0) & (x_hi == 0), -parity * wind, before)
            after = jnp.where((lane == rows_x - 1) & (x_hi == 1), swapped, after)
            curl = tile_rows(sine, 2 * ROWS // 8) * turned + half_sign * (before - after)
            for f, value in enumerate((wind, curl)):
                north, south = value[:ROWS], value[ROWS:]
                tail = 2 * LANES
                mixed = jnp.where(
                    lane_tile < LANES // 2,
                    north[:, tail : tail + LANES],
                    pltpu.roll(south[:, tail : tail + LANES], LANES // 2, 1),
                )
                tiles = (north[:, :LANES], north[:, LANES:tail], south[:, :LANES], south[:, LANES:tail], mixed)
                for b, tile in enumerate(tiles):
                    send_rows[f, b, k, half] = tile.astype(jnp.bfloat16)

    def send_half(half):
        def send_unit(block, level, sides, turn):
            owner = sides[block % 2] + lax.rem((8 * block) // 5 + turn, 8)
            return owner, pltpu.make_async_remote_copy(
                src_ref=send.at[:, block, :, half, level], dst_ref=recv.at[:, me], send_sem=send_sem, recv_sem=recv_sem,
                device_id={"lat": owner}, device_id_type=mesh_id,
            )

        def place(level):
            sides = [level * GROUP + 8 * lax.rem(level + half + p, 2) for p in range(2)]
            return sides, turn_of(level)

        for i in (4, 3, 5, 2, 6, 1, 7):
            level = lax.rem(my_level + i, HALF_LEVELS)
            sides, turn = place(level)
            for block in range(BLOCKS):
                send_unit(block, level, sides, turn)[1].start()

        sides, turn = place(my_level)
        for block in range(BLOCKS):
            owner, copy = send_unit(block, my_level, sides, turn)

            @pl.when(owner != me)
            def _():
                copy.start()

            @pl.when(owner == me)
            def _():
                pltpu.make_async_copy(send.at[:, block, :, half, my_level], recv.at[:, me], local_sem).start()

    meridional(0, u_own.reshape(SLOTS, ROWS, degrees), v_own.reshape(SLOTS, ROWS, degrees), 0, SLOTS)
    pl.semaphore_wait(ready, planes - 1)
    send_half(0)

    for i, (first, count) in enumerate(groups):
        swaps[2 * i].wait()
        swaps[2 * i + 1].wait()
        meridional(
            1, u_other.reshape(SLOTS, ROWS, degrees), v_other.reshape(SLOTS, ROWS, degrees), first, count
        )
    send_half(1)

    wave = jnp.concatenate(lane_waves, axis=1)
    end_q[...] = tile_rows(parity_of(wave), ROWS // 8).astype(jnp.bfloat16)
    turn_cos, turn_sin = cos_sin(wave * (ROWS / LON))
    turn_cos, turn_sin = tile_rows(turn_cos, ROWS // 8), tile_rows(turn_sin, ROWS // 8)
    position = lax.broadcasted_iota(jnp.int32, (ROWS, waves), 0).astype(jnp.float32)

    def advance(i, carry):
        cos, sin = carry
        rows = pl.ds(pl.multiple_of(i * ROWS, ROWS), ROWS)
        cos_q[rows, :] = cos.astype(jnp.bfloat16)
        sin_q[rows, :] = sin.astype(jnp.bfloat16)
        return cos * turn_cos - sin * turn_sin, sin * turn_cos + cos * turn_sin

    lax.fori_loop(0, half_lon // ROWS, advance, cos_sin(tile_rows(wave, ROWS // 8) * position * (1.0 / LON)))

    @pl.when(inner)
    def _():
        edge_copy(0).wait_send()
        edge_copy(1).wait_send()

    @pl.when(active)
    def _():
        remote = recv.at[:, pl.ds(0, n_lat - 1)]
        pltpu.make_async_copy(remote, remote, recv_sem).wait()
        pltpu.make_async_copy(recv.at[:, 0], recv.at[:, 0], local_sem).wait()
        recv_rows = recv.reshape(2, 2 * waves, LANES)
        for f in range(2):
            lanes = slice(f * LANES, (f + 1) * LANES)
            split[f] = recv_rows[f].astype(jnp.float32)
            cos_coeffs[:, lanes] = split[f, pl.ds(0, waves, 2), :].astype(jnp.bfloat16)
            sin_coeffs[:, lanes] = split[f, pl.ds(1, waves, 2), :].astype(jnp.bfloat16)
        step = 1280
        first_row = lax.broadcasted_iota(jnp.int32, (step, LANES), 0)

        @pl.loop(0, half_lon // step)
        def _(i):
            rows = pl.ds(pl.multiple_of(i * step, step), step)
            cos = jnp.dot(cos_q[rows, :], cos_coeffs[...], preferred_element_type=jnp.float32)
            sin = jnp.dot(sin_q[rows, :], sin_coeffs[...], preferred_element_type=jnp.float32)
            cos_u, cos_w = cos[:, :LANES], cos[:, LANES:]
            sin_u, sin_w = sin[:, :LANES], sin[:, LANES:]
            share = jnp.where(first_row + i * step == 0, 0.5, 1.0)
            cos_flux[rows, :] = (share * (cos_u * cos_w + sin_u * sin_w)).astype(jnp.bfloat16)
            sin_flux[rows, :] = (cos_u * sin_w + sin_u * cos_w).astype(jnp.bfloat16)

        end = jnp.dot(end_q[...], cos_coeffs[...], preferred_element_type=jnp.float32)
        end_flux = 0.5 * end[0:1, :LANES] * end[0:1, LANES:]

        back_rows = back.reshape(2 * waves, LANES)
        pieces = len(ORDER)
        owners = n_lat // pieces
        high = waves // pieces
        scale = 2.0 / math.sqrt(LON)

        target = ret.at[my_block, :, my_half, my_level]
        my_piece = me // owners
        my_place = lax.rem(me, owners)
        for i, offset in enumerate(ORDER):
            piece = lax.rem(my_piece + offset, pieces)
            rows = pl.ds(pl.multiple_of(piece * high, high), high)
            cos = jnp.dot(cos_k[rows, :], cos_flux[...], preferred_element_type=jnp.float32)
            sin = jnp.dot(sin_k[rows, :], sin_flux[...], preferred_element_type=jnp.float32)
            cos = cos + parity_of(row_waves[rows, :]) * end_flux
            mix[i, pl.ds(0, high, 2), :] = cos * scale
            mix[i, pl.ds(1, high, 2), :] = sin * scale
            both = pl.ds(pl.multiple_of(piece * 2 * high, 2 * high), 2 * high)
            back_rows[both, :] = mix[i].astype(jnp.bfloat16)
            if i == pieces - 1:
                pltpu.make_async_copy(back.at[me], target, back_local_sem).start()
            for j in range(1 if i == pieces - 1 else 0, owners):
                owner = piece * owners + lax.rem(my_place + j + (GROUP if i < 2 else 0), owners)
                pltpu.make_async_remote_copy(
                    src_ref=back.at[owner], dst_ref=target, send_sem=back_send_sem, recv_sem=back_recv_sem,
                    device_id={"lat": owner}, device_id_type=mesh_id,
                ).start()

        pltpu.make_async_copy(back.at[me], back.at[me], back_local_sem).wait()
        sent = recv.at[:, pl.ds(0, units - 1)]
        pltpu.make_async_copy(sent, sent, send_sem).wait()
        got = recv.at[0, pl.ds(0, units - 1)]
        pltpu.make_async_copy(got, got, back_recv_sem).wait()

    @pl.when(jnp.logical_not(active))
    def _():
        sent = recv.at[:, pl.ds(0, units)]
        pltpu.make_async_copy(sent, sent, send_sem).wait()
        got = recv.at[0, pl.ds(0, units)]
        pltpu.make_async_copy(got, got, back_recv_sem).wait()

    out_rows = out_ref.reshape(SLOTS, ROWS, degrees)
    sum_rows = sum_send.reshape(SLOTS, ROWS, degrees)
    stores = [pltpu.make_async_copy(out_ref.at[k], out_hbm.at[k], out_sem.at[k]) for k in range(SLOTS)]
    ret_rows = ret.reshape(BLOCKS, SLOTS, 2 * ROWS, LANES)
    wide_lane = lax.broadcasted_iota(jnp.int32, (2 * ROWS, LANES), 1)

    def sum_copy(k):
        return pltpu.make_async_remote_copy(
            src_ref=sum_send.at[k], dst_ref=sum_hbm.at[k],
            send_sem=sum_send_sem.at[k], recv_sem=sum_recv_sem.at[k],
            device_id={"lev": partner}, device_id_type=mesh_id,
        )

    for k in range(SLOTS):
        wave, parity, live, signed = factors(k)
        mixed = ret_rows[4, k].astype(jnp.float32)
        zero = jnp.zeros_like(mixed)
        tail_north = jnp.where(wide_lane < LANES // 2, mixed, zero).astype(jnp.bfloat16)
        tail_south = jnp.where(wide_lane < LANES // 2, pltpu.roll(mixed, LANES // 2, 1), zero).astype(jnp.bfloat16)
        north = jnp.concatenate([ret_rows[0, k], ret_rows[1, k], tail_north], axis=1)
        south = jnp.concatenate([ret_rows[2, k], ret_rows[3, k], tail_south], axis=1)
        both = jnp.dot(
            jnp.concatenate([north, south], axis=0), wide_basis[k], preferred_element_type=jnp.float32
        )
        combined = tile_rows(live, 4) * both[: 2 * ROWS] + tile_rows(signed, 4) * both[2 * ROWS :]
        sum_rows[k] = combined[ROWS:].astype(jnp.bfloat16)
        sum_copy(k).start()
        out_rows[k] = combined[:ROWS]
        stores[k].start()

    @pl.when(active)
    def _():
        sent = recv.at[0, pl.ds(0, n_lat - 1)]
        pltpu.make_async_copy(sent, sent, back_send_sem).wait()

    for k in range(SLOTS):
        stores[k].wait()
    for k in range(SLOTS):
        sum_copy(k).wait()


def body(n_lat, assign, u_spec, v_spec, basis):
    slots, lev_dev, _, degrees = u_spec.shape
    half_rows = basis.shape[1]
    waves = assign.shape[0]
    wide = 3 * LANES

    hbm = pl.BlockSpec(memory_space=pltpu.HBM)
    bf16 = jnp.bfloat16
    f32 = jnp.float32
    dma = pltpu.SemaphoreType.DMA
    own, other = pl.pallas_call(
        functools.partial(kernel, n_lat, half_rows, degrees),
        out_shape=[jax.ShapeDtypeStruct(u_spec.shape, f32), jax.ShapeDtypeStruct(u_spec.shape, bf16)],
        in_specs=[hbm] * 5,
        out_specs=[hbm, hbm],
        scratch_shapes=[
            pltpu.SMEM((waves,), jnp.int32),
            pltpu.VMEM((waves // LANES, LANES), jnp.int32),
            pltpu.VMEM((slots, lev_dev, 2, degrees), f32),
            pltpu.VMEM((slots, wide, degrees), bf16),
            pltpu.VMEM((slots, lev_dev, 2, degrees), bf16),
            pltpu.VMEM((slots, lev_dev, 2, degrees), bf16),
            pltpu.VMEM((slots, lev_dev, 2, degrees), bf16),
            pltpu.VMEM((slots, lev_dev, 2, degrees), bf16),
            pltpu.VMEM((slots, 2, degrees), bf16),
            pltpu.VMEM((slots, 2, degrees), bf16),
            pltpu.VMEM((2, BLOCKS, SLOTS, 2, HALF_LEVELS, 2, LANES), bf16),
            pltpu.VMEM((2, n_lat, SLOTS, 2, LANES), bf16),
            pltpu.VMEM((2, 2 * waves, LANES), f32),
            pltpu.VMEM((waves, 2 * LANES), bf16),
            pltpu.VMEM((waves, 2 * LANES), bf16),
            pltpu.VMEM((LON // 2, LANES), bf16),
            pltpu.VMEM((LON // 2, LANES), bf16),
            pltpu.VMEM((len(ORDER), 2 * waves // len(ORDER), LANES), f32),
            pltpu.VMEM((n_lat, SLOTS, 2, LANES), bf16),
            pltpu.VMEM((BLOCKS, SLOTS, 2, HALF_LEVELS, 2, LANES), bf16),
            pltpu.VMEM((slots, lev_dev, 2, degrees), bf16),
            pltpu.VMEM((LON // 2, waves), bf16),
            pltpu.VMEM((LON // 2, waves), bf16),
            pltpu.VMEM((ROWS, waves), bf16),
            pltpu.VMEM((waves, LON // 2), bf16),
            pltpu.VMEM((waves, LON // 2), bf16),
            pltpu.VMEM((waves, LANES), f32),
            pltpu.SemaphoreType.REGULAR,
            dma((5,)), dma((5,)), dma((5,)), dma((2,)), dma,
            dma, dma, dma, dma, dma, dma, dma((SLOTS,)), dma((SLOTS,)), dma((SLOTS,)),
        ],
        compiler_params=pltpu.CompilerParams(
            collective_id=0, has_side_effects=True, vmem_limit_bytes=67043328
        ),
    )(assign, assign.reshape(waves // LANES, LANES), u_spec, v_spec, basis)
    return own + other.astype(f32)


def solution(mesh):
    return jax.shard_map(
        functools.partial(body, mesh.shape["lat"]),
        mesh=mesh,
        in_specs=(
            P(),
            P("lat", "lev", None, None),
            P("lat", "lev", None, None),
            P("lat", "lev", None),
        ),
        out_specs=P("lat", "lev", None, None),
        check_vma=False,
    )
```

```python
import functools
import math

import jax
import jax.numpy as jnp
from jax import lax
from jax.experimental import pallas as pl
from jax.experimental.pallas import tpu as pltpu
from jax.sharding import PartitionSpec as P

LON = 2560
SLOTS = 5
BLOCKS = 5
LANES = 128
GROUP = 16
HALF_LEVELS = 8
ORDER = (2, 1, 3, 0)
ROWS = 16


def cos_sin(turns):
    x = turns - jnp.floor(turns + 0.5)
    u = x * x
    cos = jnp.full_like(u, (2 * math.pi) ** 18 / math.factorial(18) * -1.0)
    sin = jnp.full_like(u, (2 * math.pi) ** 19 / math.factorial(19) * -1.0)
    for i in range(8, -1, -1):
        sign = 1.0 if i % 2 == 0 else -1.0
        cos = cos * u + sign * (2 * math.pi) ** (2 * i) / math.factorial(2 * i)
        sin = sin * u + sign * (2 * math.pi) ** (2 * i + 1) / math.factorial(2 * i + 1)
    return cos, sin * x


def tile_rows(value, count):
    return jnp.concatenate([value] * count, axis=0)


def parity_of(wave):
    return 1.0 - 2.0 * (wave - 2.0 * jnp.floor(0.5 * wave))


def kernel(
    n_lat, half_rows, degrees,
    assign_hbm, lanes_hbm, u_ref, v_ref, basis_ref,
    out_hbm, sum_hbm,
    assign_ref, assign_lanes_ref, out_ref,
    wide_basis, u_own, v_own, u_other, v_other, edge_send, edge_recv,
    send, recv, split, cos_coeffs, sin_coeffs, cos_flux, sin_flux, mix, back, ret, sum_send,
    cos_q, sin_q, end_q, cos_k, sin_k, row_waves,
    ready, load_sem, swap_send_sem, swap_recv_sem, edge_send_sem, edge_recv_sem,
    send_sem, recv_sem, local_sem, back_send_sem, back_recv_sem, back_local_sem, sum_send_sem, sum_recv_sem, out_sem,
):
    me = lax.axis_index("lat")
    lev = lax.axis_index("lev")
    x_hi = lev // 2
    core = lax.rem(lev, 2)
    rows_x = 2 * half_rows
    wide = wide_basis.shape[1]
    waves = SLOTS * n_lat
    half_lon = LON // 2
    units = BLOCKS * GROUP
    mesh_id = pl.DeviceIdType.MESH

    def turn_of(level):
        return lax.rem(5 * level + 4 * core, 8)

    my_level = me // GROUP
    my_z = lax.rem(lax.rem(me, 8) + 8 - turn_of(my_level), 8)
    my_block = (5 * my_z + 7) // 8
    active = (8 * my_block) // 5 == my_z
    my_half = lax.rem(lax.rem(me // 8, 2) + my_block + my_level, 2)

    own_rows = pl.ds(pl.multiple_of(core * half_rows, ROWS), half_rows)
    loads = [
        pltpu.make_async_copy(basis_ref, wide_basis.at[:, own_rows], load_sem.at[0]),
        pltpu.make_async_copy(u_ref, u_own, load_sem.at[1]),
        pltpu.make_async_copy(v_ref, v_own, load_sem.at[2]),
        pltpu.make_async_copy(assign_hbm, assign_ref, load_sem.at[3]),
        pltpu.make_async_copy(lanes_hbm, assign_lanes_ref, load_sem.at[4]),
    ]
    for load in loads:
        load.start()

    barrier = pltpu.get_barrier_semaphore()
    for i in range(1, 4):
        pl.semaphore_signal(barrier, inc=1, device_id={"lev": lax.rem(lev + i, 4)}, device_id_type=mesh_id)
    plane = me - lax.rem(me, GROUP)

    @pl.loop(1, GROUP)
    def _(i):
        peer = plane + lax.rem(me + i, GROUP)
        pl.semaphore_signal(barrier, inc=1, device_id={"lat": peer}, device_id_type=mesh_id)

    planes = n_lat // GROUP

    @pl.loop(1, planes)
    def _(i):
        peer = lax.rem(me + i * GROUP, n_lat)
        pl.semaphore_signal(barrier, inc=1, device_id={"lat": peer}, device_id_type=mesh_id)

    inner = x_hi + core == 1
    loads[0].wait()

    @pl.when(inner & (x_hi == 1))
    def _():
        for k in range(SLOTS):
            edge_send[k] = jnp.broadcast_to(wide_basis[k, 0:ROWS, :][0:1], (2, degrees))

    @pl.when(inner & (x_hi == 0))
    def _():
        for k in range(SLOTS):
            edge_send[k] = jnp.broadcast_to(wide_basis[k, rows_x - ROWS : rows_x, :][ROWS - 1 :], (2, degrees))

    pl.semaphore_wait(barrier, 3 + GROUP - 1 + planes - 1)

    partner = lax.rem(lev + 2, 4)
    sibling = 2 * x_hi + 1 - core

    def swap(i, source, target, device):
        return pltpu.make_async_remote_copy(
            src_ref=source, dst_ref=target, send_sem=swap_send_sem.at[i], recv_sem=swap_recv_sem.at[i],
            device_id={"lev": device}, device_id_type=mesh_id,
        )

    groups = ((0, 4), (4, 1))
    swaps = [
        swap(2 * i + j, own.at[pl.ds(first, count)], other.at[pl.ds(first, count)], partner)
        for i, (first, count) in enumerate(groups)
        for j, (own, other) in enumerate(((u_own, u_other), (v_own, v_other)))
    ]
    swap_basis = swap(4, wide_basis.at[:, own_rows], wide_basis.at[:, own_rows], sibling)

    edge_base = 2 - 2 * x_hi

    def edge_copy(i):
        return pltpu.make_async_remote_copy(
            src_ref=edge_send, dst_ref=edge_recv, send_sem=edge_send_sem.at[i], recv_sem=edge_recv_sem,
            device_id={"lev": edge_base + i}, device_id_type=mesh_id,
        )

    @pl.when(inner)
    def _():
        edge_copy(0).start()
        edge_copy(1).start()

    swap_basis.start()
    @pl.loop(1, planes)
    def _(i):
        peer = lax.rem(me + i * GROUP, n_lat)
        pl.semaphore_signal(ready, inc=1, device_id={"lat": peer}, device_id_type=mesh_id)

    loads[1].wait()
    loads[2].wait()
    for copy in swaps:
        copy.start()
    loads[3].wait()
    loads[4].wait()

    lane_waves = []
    for t in range(waves // LANES):
        line = assign_lanes_ref[t : t + 1, :].astype(jnp.float32)
        lane_waves.append(jnp.broadcast_to(line, (8, LANES)))
        row_waves[t * LANES : (t + 1) * LANES, :] = jnp.broadcast_to(line, (LANES, LANES)).T

    chunk = 64

    @pl.loop(0, waves // chunk)
    def _(i):
        rows = pl.ds(pl.multiple_of(i * chunk, chunk), chunk)
        wave = row_waves[rows, :]
        column = lax.broadcasted_iota(jnp.int32, (chunk, LANES), 1).astype(jnp.float32)
        cos, sin = cos_sin(wave * column * (1.0 / LON))
        turn_cos, turn_sin = cos_sin(wave * (LANES / LON))
        for step in range(half_lon // LANES):
            lanes = slice(step * LANES, (step + 1) * LANES)
            cos_k[rows, lanes] = cos.astype(jnp.bfloat16)
            sin_k[rows, lanes] = sin.astype(jnp.bfloat16)
            cos, sin = cos * turn_cos - sin * turn_sin, sin * turn_cos + cos * turn_sin

    edge_copy(0).wait_recv()
    for k in range(SLOTS):
        wide_basis[k, rows_x:wide, :] = jnp.broadcast_to(edge_recv[k][0:1], (wide - rows_x, degrees))
    swap_basis.wait()

    send_rows = send.reshape(2, BLOCKS, SLOTS, 2, ROWS, LANES)
    lane = lax.broadcasted_iota(jnp.int32, (2 * ROWS, wide), 1)
    row = lax.broadcasted_iota(jnp.int32, (2 * ROWS, wide), 0)
    half_sign = jnp.where(row < ROWS, -0.5, 0.5)
    even = lax.rem(row, 2) == 0
    lane_tile = lax.broadcasted_iota(jnp.int32, (ROWS, LANES), 1)
    degree = lax.broadcasted_iota(jnp.int32, (8, degrees), 1)
    degree_sign = (1 - 2 * lax.rem(degree, 2)).astype(jnp.float32)

    def factors(k):
        wave = assign_ref[me * SLOTS + k]
        parity = (1 - 2 * lax.rem(wave, 2)).astype(jnp.float32)
        live = jnp.where(degree >= wave, 1.0, 0.0)
        return wave, parity, live, live * (parity * degree_sign)

    def meridional(half, u_rows, v_rows, first, count):
        for k in range(first, first + count):
            wave, parity, live, signed = factors(k)
            live = tile_rows(live, 2).astype(jnp.bfloat16)
            signed = tile_rows(signed, 2).astype(jnp.bfloat16)
            u, v = u_rows[k], v_rows[k]
            lhs = jnp.concatenate([u * live, u * signed, v * live, v * signed], axis=0)
            fields = lax.dot_general(
                wide_basis[k], lhs, (((1,), (1,)), ((), ())), preferred_element_type=jnp.float32
            ).T
            wind, other = fields[: 2 * ROWS], fields[2 * ROWS :]
            turned = jnp.where(even, pltpu.roll(other, 2 * ROWS - 1, 0), -pltpu.roll(other, 1, 0))
            sine = cos_sin(jnp.full((8, wide), 1.0 / LON, jnp.float32) * wave.astype(jnp.float32))[1]
            before = pltpu.roll(wind, 1, 1)
            after = pltpu.roll(wind, wide - 1, 1)
            swapped = jnp.concatenate([wind[ROWS:], wind[:ROWS]], axis=0)
            before = jnp.where((lane == 0) & (x_hi == 0), -parity * wind, before)
            after = jnp.where((lane == rows_x - 1) & (x_hi == 1), swapped, after)
            curl = tile_rows(sine, 2 * ROWS // 8) * turned + half_sign * (before - after)
            for f, value in enumerate((wind, curl)):
                north, south = value[:ROWS], value[ROWS:]
                tail = 2 * LANES
                mixed = jnp.where(
                    lane_tile < LANES // 2,
                    north[:, tail : tail + LANES],
                    pltpu.roll(south[:, tail : tail + LANES], LANES // 2, 1),
                )
                tiles = (north[:, :LANES], north[:, LANES:tail], south[:, :LANES], south[:, LANES:tail], mixed)
                for b, tile in enumerate(tiles):
                    send_rows[f, b, k, half] = tile.astype(jnp.bfloat16)

    def send_half(half):
        def send_unit(block, level, sides, turn):
            owner = sides[block % 2] + lax.rem((8 * block) // 5 + turn, 8)
            return owner, pltpu.make_async_remote_copy(
                src_ref=send.at[:, block, :, half, level], dst_ref=recv.at[:, me], send_sem=send_sem, recv_sem=recv_sem,
                device_id={"lat": owner}, device_id_type=mesh_id,
            )

        def place(level):
            sides = [level * GROUP + 8 * lax.rem(level + half + p, 2) for p in range(2)]
            return sides, turn_of(level)

        for i in ((4, 3, 5, 2, 6, 1, 7) if half == 0 else (4, 5, 3, 6, 2, 7, 1)):
            level = lax.rem(my_level + i, HALF_LEVELS)
            sides, turn = place(level)
            for block in range(BLOCKS):
                send_unit(block, level, sides, turn)[1].start()

        sides, turn = place(my_level)
        for block in range(BLOCKS):
            owner, copy = send_unit(block, my_level, sides, turn)

            @pl.when(owner != me)
            def _():
                copy.start()

            @pl.when(owner == me)
            def _():
                pltpu.make_async_copy(send.at[:, block, :, half, my_level], recv.at[:, me], local_sem).start()

    meridional(0, u_own.reshape(SLOTS, ROWS, degrees), v_own.reshape(SLOTS, ROWS, degrees), 0, SLOTS)
    pl.semaphore_wait(ready, planes - 1)
    send_half(0)

    for i, (first, count) in enumerate(groups):
        swaps[2 * i].wait()
        swaps[2 * i + 1].wait()
        meridional(
            1, u_other.reshape(SLOTS, ROWS, degrees), v_other.reshape(SLOTS, ROWS, degrees), first, count
        )
    send_half(1)

    wave = jnp.concatenate(lane_waves, axis=1)
    end_q[...] = tile_rows(parity_of(wave), ROWS // 8).astype(jnp.bfloat16)
    turn_cos, turn_sin = cos_sin(wave * (ROWS / LON))
    turn_cos, turn_sin = tile_rows(turn_cos, ROWS // 8), tile_rows(turn_sin, ROWS // 8)
    position = lax.broadcasted_iota(jnp.int32, (ROWS, waves), 0).astype(jnp.float32)

    def advance(i, carry):
        cos, sin = carry
        rows = pl.ds(pl.multiple_of(i * ROWS, ROWS), ROWS)
        cos_q[rows, :] = cos.astype(jnp.bfloat16)
        sin_q[rows, :] = sin.astype(jnp.bfloat16)
        return cos * turn_cos - sin * turn_sin, sin * turn_cos + cos * turn_sin

    lax.fori_loop(0, half_lon // ROWS, advance, cos_sin(tile_rows(wave, ROWS // 8) * position * (1.0 / LON)))

    @pl.when(inner)
    def _():
        edge_copy(0).wait_send()
        edge_copy(1).wait_send()

    @pl.when(active)
    def _():
        remote = recv.at[:, pl.ds(0, n_lat - 1)]
        pltpu.make_async_copy(remote, remote, recv_sem).wait()
        pltpu.make_async_copy(recv.at[:, 0], recv.at[:, 0], local_sem).wait()
        recv_rows = recv.reshape(2, 2 * waves, LANES)
        for f in range(2):
            lanes = slice(f * LANES, (f + 1) * LANES)
            split[f] = recv_rows[f].astype(jnp.float32)
            cos_coeffs[:, lanes] = split[f, pl.ds(0, waves, 2), :].astype(jnp.bfloat16)
            sin_coeffs[:, lanes] = split[f, pl.ds(1, waves, 2), :].astype(jnp.bfloat16)
        step = 1280
        first_row = lax.broadcasted_iota(jnp.int32, (step, LANES), 0)

        @pl.loop(0, half_lon // step)
        def _(i):
            rows = pl.ds(pl.multiple_of(i * step, step), step)
            cos = jnp.dot(cos_q[rows, :], cos_coeffs[...], preferred_element_type=jnp.float32)
            sin = jnp.dot(sin_q[rows, :], sin_coeffs[...], preferred_element_type=jnp.float32)
            cos_u, cos_w = cos[:, :LANES], cos[:, LANES:]
            sin_u, sin_w = sin[:, :LANES], sin[:, LANES:]
            share = jnp.where(first_row + i * step == 0, 0.5, 1.0)
            cos_flux[rows, :] = (share * (cos_u * cos_w + sin_u * sin_w)).astype(jnp.bfloat16)
            sin_flux[rows, :] = (cos_u * sin_w + sin_u * cos_w).astype(jnp.bfloat16)

        end = jnp.dot(end_q[...], cos_coeffs[...], preferred_element_type=jnp.float32)
        end_flux = 0.5 * end[0:1, :LANES] * end[0:1, LANES:]

        back_rows = back.reshape(2 * waves, LANES)
        pieces = len(ORDER)
        owners = n_lat // pieces
        high = waves // pieces
        scale = 2.0 / math.sqrt(LON)

        target = ret.at[my_block, :, my_half, my_level]
        my_piece = me // owners
        my_place = lax.rem(me, owners)
        for i, offset in enumerate(ORDER):
            piece = lax.rem(my_piece + offset, pieces)
            rows = pl.ds(pl.multiple_of(piece * high, high), high)
            cos = jnp.dot(cos_k[rows, :], cos_flux[...], preferred_element_type=jnp.float32)
            sin = jnp.dot(sin_k[rows, :], sin_flux[...], preferred_element_type=jnp.float32)
            cos = cos + parity_of(row_waves[rows, :]) * end_flux
            mix[i, pl.ds(0, high, 2), :] = cos * scale
            mix[i, pl.ds(1, high, 2), :] = sin * scale
            both = pl.ds(pl.multiple_of(piece * 2 * high, 2 * high), 2 * high)
            back_rows[both, :] = mix[i].astype(jnp.bfloat16)
            if i == pieces - 1:
                pltpu.make_async_copy(back.at[me], target, back_local_sem).start()
            for j in range(1 if i == pieces - 1 else 0, owners):
                owner = piece * owners + lax.rem(my_place + j + (GROUP if i < 2 else 0), owners)
                pltpu.make_async_remote_copy(
                    src_ref=back.at[owner], dst_ref=target, send_sem=back_send_sem, recv_sem=back_recv_sem,
                    device_id={"lat": owner}, device_id_type=mesh_id,
                ).start()

        pltpu.make_async_copy(back.at[me], back.at[me], back_local_sem).wait()
        sent = recv.at[:, pl.ds(0, units - 1)]
        pltpu.make_async_copy(sent, sent, send_sem).wait()
        got = recv.at[0, pl.ds(0, units - 1)]
        pltpu.make_async_copy(got, got, back_recv_sem).wait()

    @pl.when(jnp.logical_not(active))
    def _():
        sent = recv.at[:, pl.ds(0, units)]
        pltpu.make_async_copy(sent, sent, send_sem).wait()
        got = recv.at[0, pl.ds(0, units)]
        pltpu.make_async_copy(got, got, back_recv_sem).wait()

    out_rows = out_ref.reshape(SLOTS, ROWS, degrees)
    sum_rows = sum_send.reshape(SLOTS, ROWS, degrees)
    stores = [pltpu.make_async_copy(out_ref.at[k], out_hbm.at[k], out_sem.at[k]) for k in range(SLOTS)]
    ret_rows = ret.reshape(BLOCKS, SLOTS, 2 * ROWS, LANES)
    wide_lane = lax.broadcasted_iota(jnp.int32, (2 * ROWS, LANES), 1)

    def sum_copy(k):
        return pltpu.make_async_remote_copy(
            src_ref=sum_send.at[k], dst_ref=sum_hbm.at[k],
            send_sem=sum_send_sem.at[k], recv_sem=sum_recv_sem.at[k],
            device_id={"lev": partner}, device_id_type=mesh_id,
        )

    for k in range(SLOTS):
        wave, parity, live, signed = factors(k)
        mixed = ret_rows[4, k].astype(jnp.float32)
        zero = jnp.zeros_like(mixed)
        tail_north = jnp.where(wide_lane < LANES // 2, mixed, zero).astype(jnp.bfloat16)
        tail_south = jnp.where(wide_lane < LANES // 2, pltpu.roll(mixed, LANES // 2, 1), zero).astype(jnp.bfloat16)
        north = jnp.concatenate([ret_rows[0, k], ret_rows[1, k], tail_north], axis=1)
        south = jnp.concatenate([ret_rows[2, k], ret_rows[3, k], tail_south], axis=1)
        both = jnp.dot(
            jnp.concatenate([north, south], axis=0), wide_basis[k], preferred_element_type=jnp.float32
        )
        combined = tile_rows(live, 4) * both[: 2 * ROWS] + tile_rows(signed, 4) * both[2 * ROWS :]
        sum_rows[k] = combined[ROWS:].astype(jnp.bfloat16)
        sum_copy(k).start()
        out_rows[k] = combined[:ROWS]
        stores[k].start()

    @pl.when(active)
    def _():
        sent = recv.at[0, pl.ds(0, n_lat - 1)]
        pltpu.make_async_copy(sent, sent, back_send_sem).wait()

    for k in range(SLOTS):
        stores[k].wait()
    for k in range(SLOTS):
        sum_copy(k).wait()


def body(n_lat, assign, u_spec, v_spec, basis):
    slots, lev_dev, _, degrees = u_spec.shape
    half_rows = basis.shape[1]
    waves = assign.shape[0]
    wide = 3 * LANES

    hbm = pl.BlockSpec(memory_space=pltpu.HBM)
    bf16 = jnp.bfloat16
    f32 = jnp.float32
    dma = pltpu.SemaphoreType.DMA
    own, other = pl.pallas_call(
        functools.partial(kernel, n_lat, half_rows, degrees),
        out_shape=[jax.ShapeDtypeStruct(u_spec.shape, f32), jax.ShapeDtypeStruct(u_spec.shape, bf16)],
        in_specs=[hbm] * 5,
        out_specs=[hbm, hbm],
        scratch_shapes=[
            pltpu.SMEM((waves,), jnp.int32),
            pltpu.VMEM((waves // LANES, LANES), jnp.int32),
            pltpu.VMEM((slots, lev_dev, 2, degrees), f32),
            pltpu.VMEM((slots, wide, degrees), bf16),
            pltpu.VMEM((slots, lev_dev, 2, degrees), bf16),
            pltpu.VMEM((slots, lev_dev, 2, degrees), bf16),
            pltpu.VMEM((slots, lev_dev, 2, degrees), bf16),
            pltpu.VMEM((slots, lev_dev, 2, degrees), bf16),
            pltpu.VMEM((slots, 2, degrees), bf16),
            pltpu.VMEM((slots, 2, degrees), bf16),
            pltpu.VMEM((2, BLOCKS, SLOTS, 2, HALF_LEVELS, 2, LANES), bf16),
            pltpu.VMEM((2, n_lat, SLOTS, 2, LANES), bf16),
            pltpu.VMEM((2, 2 * waves, LANES), f32),
            pltpu.VMEM((waves, 2 * LANES), bf16),
            pltpu.VMEM((waves, 2 * LANES), bf16),
            pltpu.VMEM((LON // 2, LANES), bf16),
            pltpu.VMEM((LON // 2, LANES), bf16),
            pltpu.VMEM((len(ORDER), 2 * waves // len(ORDER), LANES), f32),
            pltpu.VMEM((n_lat, SLOTS, 2, LANES), bf16),
            pltpu.VMEM((BLOCKS, SLOTS, 2, HALF_LEVELS, 2, LANES), bf16),
            pltpu.VMEM((slots, lev_dev, 2, degrees), bf16),
            pltpu.VMEM((LON // 2, waves), bf16),
            pltpu.VMEM((LON // 2, waves), bf16),
            pltpu.VMEM((ROWS, waves), bf16),
            pltpu.VMEM((waves, LON // 2), bf16),
            pltpu.VMEM((waves, LON // 2), bf16),
            pltpu.VMEM((waves, LANES), f32),
            pltpu.SemaphoreType.REGULAR,
            dma((5,)), dma((5,)), dma((5,)), dma((2,)), dma,
            dma, dma, dma, dma, dma, dma, dma((SLOTS,)), dma((SLOTS,)), dma((SLOTS,)),
        ],
        compiler_params=pltpu.CompilerParams(
            collective_id=0, has_side_effects=True, vmem_limit_bytes=67043328
        ),
    )(assign, assign.reshape(waves // LANES, LANES), u_spec, v_spec, basis)
    return own + other.astype(f32)


def solution(mesh):
    return jax.shard_map(
        functools.partial(body, mesh.shape["lat"]),
        mesh=mesh,
        in_specs=(
            P(),
            P("lat", "lev", None, None),
            P("lat", "lev", None, None),
            P("lat", "lev", None),
        ),
        out_specs=P("lat", "lev", None, None),
        check_vma=False,
    )
```
